16 devices in a mesh: dp: 2 (over y, z), tp: 8 (over x, core).
Axes of the slice: x: 4, y: 2, z: 1, core: 2. Of those that a mesh axis runs over, the one named last changes fastest.
The devices are a block of a 4x4x8 slice.
Arguments:
- act_in: bfloat16 [16, 1024, 2560], P('dp'), parts along dimension 0
- ln_gain: float32 [2, 2560], replicated
- ln_bias: float32 [2, 2560], replicated
- w_qkv: bfloat16 [2, 2560, 32, 240], P(None, None, 'tp')
- w_out: bfloat16 [2, 2560, 2560], P(None, 'tp')
- w_up: bfloat16 [2, 2560, 10240], P(None, None, 'tp')
- w_down: bfloat16 [2, 10240, 2560], P(None, 'tp')
Outputs:
- output: bfloat16 [16, 1024, 2560], P('dp'), parts along dimension 0
There are 2 independent parts. The reference program is written for one: setup_inputs(seed, part) draws one part's arguments, and reference() takes and returns one part's arrays. A program takes and returns all parts, laid end to end along the dimension named above; an argument that names none is the same for every part.
All inputs are finite; a program needn't handle non-finite values.
Results may differ from the reference program's by a relative error of at most 0.0174878.
Values are sent between devices in bfloat16 or wider.
A program may use at most 768 MiB of HBM per device.

```python
import math
import jax
import jax.numpy as jnp
from jax import lax

D_MODEL = 2560
HEADS = 32
KV_HEADS = 32
HEAD_DIM = 80
FF_DIM = 10240
BATCH = 8
SEQ_LEN = 1024
LAYERS = 2

GROUP_HEADS = HEADS // KV_HEADS
LN_EPS = 1e-5
ROPE_BASE = 10000.0
QUERY_GAIN = 2.0


def setup_inputs(seed: int = 0, part: int = 0) -> dict:
    base_key = jax.random.key(seed)
    part_key = jax.random.fold_in(base_key, part)
    key_list = jax.random.split(base_key, 6)
    group_cols = (GROUP_HEADS + 2) * HEAD_DIM
    col_gain = jnp.where(jnp.arange(group_cols) < GROUP_HEADS * HEAD_DIM, QUERY_GAIN, 1.0)
    act_in = jax.random.normal(part_key, (BATCH, SEQ_LEN, D_MODEL), jnp.float32)
    ln_gain = 1.0 + 0.2 * jax.random.normal(key_list[0], (LAYERS, D_MODEL), jnp.float32)
    ln_bias = 0.3 * jax.random.normal(key_list[1], (LAYERS, D_MODEL), jnp.float32)
    w_qkv = jax.random.normal(key_list[2], (LAYERS, D_MODEL, KV_HEADS, group_cols), jnp.float32) * col_gain * D_MODEL ** -0.5
    w_out = jax.random.normal(key_list[3], (LAYERS, HEADS * HEAD_DIM, D_MODEL), jnp.float32) * (1.5 * (HEADS * HEAD_DIM) ** -0.5)
    w_up = jax.random.normal(key_list[4], (LAYERS, D_MODEL, FF_DIM), jnp.float32) * D_MODEL ** -0.5
    w_down = jax.random.normal(key_list[5], (LAYERS, FF_DIM, D_MODEL), jnp.float32) * FF_DIM ** -0.5
    return {"act_in": act_in.astype(jnp.bfloat16), "ln_gain": ln_gain, "ln_bias": ln_bias, "w_qkv": w_qkv.astype(jnp.bfloat16), "w_out": w_out.astype(jnp.bfloat16), "w_up": w_up.astype(jnp.bfloat16), "w_down": w_down.astype(jnp.bfloat16)}


def layer_norm(hidden, gain, bias):
    hidden_f = hidden.astype(jnp.float32)
    row_mean = jnp.mean(hidden_f, axis=-1, keepdims=True)
    centered = hidden_f - row_mean
    row_var = jnp.mean(centered * centered, axis=-1, keepdims=True)
    return (centered * lax.rsqrt(row_var + LN_EPS) * gain + bias).astype(jnp.bfloat16)


def rope_tables():
    half_dim = HEAD_DIM // 2
    inv_freq = ROPE_BASE ** (-2.0 * jnp.arange(half_dim, dtype=jnp.float32) / HEAD_DIM)
    angles = jnp.arange(SEQ_LEN, dtype=jnp.float32)[:, None] * inv_freq[None, :]
    return jnp.cos(angles), jnp.sin(angles)


def apply_rope(proj, cos_tab, sin_tab):
    half_dim = proj.shape[-1] // 2
    first = proj[..., :half_dim]
    second = proj[..., half_dim:]
    return jnp.concatenate([first * cos_tab - second * sin_tab, second * cos_tab + first * sin_tab], axis=-1)


def attend_sequence(operands):
    query, keys, values = operands
    scores = jnp.einsum("sgrd,tgd->grst", query.astype(jnp.float32), keys.astype(jnp.float32)) / math.sqrt(HEAD_DIM)
    positions = jnp.arange(SEQ_LEN)
    allowed = positions[:, None] >= positions[None, :]
    scores = jnp.where(allowed, scores, -1e30)
    attn_probs = jax.nn.softmax(scores, axis=-1).astype(jnp.bfloat16)
    context = jnp.einsum("grst,tgd->sgrd", attn_probs.astype(jnp.float32), values.astype(jnp.float32))
    return context.astype(jnp.bfloat16)


def layer_step(hidden, params):
    gain, bias, w_qkv, w_out, w_up, w_down = params
    normed = layer_norm(hidden, gain, bias)
    flat = normed.reshape(BATCH * SEQ_LEN, D_MODEL)
    qkv_proj = jnp.dot(flat, w_qkv.reshape(D_MODEL, -1), preferred_element_type=jnp.float32)
    qkv_proj = qkv_proj.reshape(BATCH, SEQ_LEN, KV_HEADS, GROUP_HEADS + 2, HEAD_DIM)
    cos_tab, sin_tab = rope_tables()
    query = apply_rope(qkv_proj[:, :, :, :GROUP_HEADS], cos_tab[None, :, None, None, :], sin_tab[None, :, None, None, :]).astype(jnp.bfloat16)
    keys = apply_rope(qkv_proj[:, :, :, GROUP_HEADS], cos_tab[None, :, None, :], sin_tab[None, :, None, :]).astype(jnp.bfloat16)
    values = qkv_proj[:, :, :, GROUP_HEADS + 1].astype(jnp.bfloat16)
    context = lax.map(attend_sequence, (query, keys, values))
    attn_part = jnp.dot(context.reshape(BATCH * SEQ_LEN, HEADS * HEAD_DIM), w_out, preferred_element_type=jnp.float32)
    up_proj = jnp.dot(flat, w_up, preferred_element_type=jnp.float32)
    gelu_out = jax.nn.gelu(up_proj, approximate=False).astype(jnp.bfloat16)
    mlp_part = jnp.dot(gelu_out, w_down, preferred_element_type=jnp.float32)
    update = (attn_part + mlp_part).astype(jnp.bfloat16).reshape(BATCH, SEQ_LEN, D_MODEL)
    new_hidden = (hidden.astype(jnp.float32) + update.astype(jnp.float32)).astype(jnp.bfloat16)
    return new_hidden, None


def reference(act_in, ln_gain, ln_bias, w_qkv, w_out, w_up, w_down):
    act_out = lax.scan(layer_step, act_in, (ln_gain, ln_bias, w_qkv, w_out, w_up, w_down))[0]
    return act_out
```

```python
import functools

import jax
import jax.numpy as jnp
import numpy as np
from jax import lax
from jax.experimental import pallas as pl
from jax.experimental.pallas import tpu as pltpu
from jax.sharding import PartitionSpec as P

LN_EPS = 1e-5
ROPE_BASE = 10000.0
F32 = jnp.float32
BF16 = jnp.bfloat16
MESH = pl.DeviceIdType.MESH
VMEM_LIMIT = 67043328

CORES = 2
ROWS = 256
LANES = 128
SLOT = 40


def rope_tables(seq_len, head_dim):
    half_dim = head_dim // 2
    inv_freq = (ROPE_BASE ** (-2.0 * np.arange(half_dim, dtype=np.float32) / head_dim)).astype(np.float32)
    angles = np.arange(seq_len, dtype=np.float32)[:, None] * inv_freq[None, :]
    cos_tab = np.ones((seq_len, LANES), np.float32)
    sin_tab = np.zeros((seq_len, LANES), np.float32)
    for k in range(2):
        cos_tab[:, k * half_dim:(k + 1) * half_dim] = np.cos(angles)
        sin_tab[:, k * half_dim:(k + 1) * half_dim] = np.sin(angles)
    return cos_tab, sin_tab


def prep_qkv(w_qkv, head_dim):
    layers, d_model, heads, _ = w_qkv.shape
    half_dim = head_dim // 2
    w = w_qkv.reshape(layers, d_model, heads, 3, 2, half_dim)
    w = jnp.transpose(w, (0, 2, 1, 4, 3, 5)).reshape(layers, heads, d_model, 2, 3 * half_dim)
    w = jnp.pad(w, ((0, 0),) * 4 + ((0, LANES - 3 * half_dim),))
    return w.reshape(layers, heads, d_model, 2 * LANES)


def prep_out(w_out, heads, head_dim):
    layers, _, d_model = w_out.shape
    half_dim = head_dim // 2
    w = w_out.reshape(layers, heads, 2, half_dim, d_model)
    first = jnp.transpose(w[:, :3], (0, 2, 1, 3, 4)).reshape(layers, 2, 3 * half_dim, d_model)
    first = jnp.pad(first, ((0, 0), (0, 0), (0, LANES - 3 * half_dim), (0, 0)))
    second = jnp.pad(w[:, 3], ((0, 0), (0, 0), (half_dim, LANES - 2 * half_dim), (0, 0)))
    return jnp.concatenate([first, second], axis=1).reshape(layers, 4 * LANES, d_model)


def body(cfg, act, w_q, w_o, w_u, w_d, gain, bias, cos_v, sin_v,
         out, st_q, st_o, st_u, st_d,
         x_v, n_v, q_v, kv_v, cu_v, p_v, wq_v, wu_v, wod_v,
         a1r, a2r, br, comb, ysh, xres,
         s_a1s, s_a1r, s_a2s, s_a2r, s_bs, s_br, s_cs, s_cr, s_ds, s_dr, s_yl, s_x, s_xr, s_f, s_wl, s_ws, s_wr):
    n_chip, layers, heads, head_dim, d_model, ff, items, blocks = cfg
    seq_blocks = blocks
    half_dim = head_dim // 2
    total = layers * items
    tp = lax.axis_index("tp")
    chip = lax.div(tp, CORES)
    core = lax.rem(tp, CORES)
    right = {"tp": lax.rem(chip + 1, n_chip) * CORES + core}
    left = {"tp": lax.rem(chip + n_chip - 1, n_chip) * CORES + core}
    mate = {"tp": chip * CORES + (CORES - 1 - core)}
    own_base = core * (items * ROWS)
    shard = ROWS // n_chip
    hs = shard // 2
    ow = 4 * LANES

    def ring(k):
        return lax.rem(chip + k, n_chip)

    def remote(src, dst, ssem, rsem, dev):
        return pltpu.make_async_remote_copy(src_ref=src, dst_ref=dst, send_sem=ssem, recv_sem=rsem, device_id=dev, device_id_type=MESH)

    def sh_rows(k, off, size):
        return pl.ds(pl.multiple_of(ring(k) * shard + off, hs), size)

    def y_rows(t, k, off, size):
        base = own_base + lax.rem(t, items) * ROWS
        return pl.ds(pl.multiple_of(base + ring(k) * shard + off, hs), size)

    def item_rows(t):
        return pl.ds(pl.multiple_of(own_base + lax.rem(t, items) * ROWS, ROWS), ROWS)

    def w_dst(h):
        return [wq_v.at[pl.ds(h * heads, heads)], wu_v.at[h], wod_v.at[pl.ds(h * ow, ow)], wod_v.at[pl.ds(2 * ow + h * ff, ff)]]

    def w_src(l):
        return [w_q.at[l], w_u.at[l], w_o.at[l], w_d.at[l]]

    staged = [st_q, st_u, st_o, st_d]

    def own_load(l):
        return [pltpu.make_async_copy(s, d, s_wl.at[0, i]) for i, (s, d) in enumerate(zip(w_src(l), w_dst(0)))]

    def mate_load():
        return [pltpu.make_async_copy(s, d, s_wl.at[1, i]) for i, (s, d) in enumerate(zip(staged, w_dst(1)))]

    def push_first():
        return [remote(s, d, s_ws.at[0, i], s_wr.at[0, i], mate) for i, (s, d) in enumerate(zip(w_src(0), w_dst(1)))]

    def push_second():
        return [remote(s, d, s_ws.at[1, i], s_wr.at[1, i], mate) for i, (s, d) in enumerate(zip(w_src(1), staged))]

    def wait_weights(t, idx):
        @pl.when(t == 0)
        def _():
            for i in idx:
                own_load(0)[i].wait()
                push_first()[i].wait_recv()

        @pl.when(t == items)
        def _():
            for i in idx:
                own_load(1)[i].wait()
                mate_load()[i].wait()

    def x_load(t):
        @pl.when(t < items)
        def _():
            pltpu.make_async_copy(act.at[item_rows(t)], x_v, s_x).start()

        @pl.when(t >= items)
        def _():
            pltpu.make_async_copy(out.at[item_rows(t)], x_v, s_x).start()

    def x_wait():
        pltpu.make_async_copy(act.at[pl.ds(0, ROWS)], x_v, s_x).wait()

    def xres_load(t):
        sl = lax.rem(t, 2)

        @pl.when(t < items)
        def _():
            pltpu.make_async_copy(act.at[y_rows(t, 0, 0, shard)], xres.at[sl], s_xr.at[sl]).start()

        @pl.when(t >= items)
        def _():
            pltpu.make_async_copy(out.at[y_rows(t, 0, 0, shard)], xres.at[sl], s_xr.at[sl]).start()

    def xres_wait(t):
        sl = lax.rem(t, 2)
        pltpu.make_async_copy(act.at[pl.ds(0, shard)], xres.at[sl], s_xr.at[sl]).wait()

    def a_copies(t):
        sl, s3 = lax.rem(t, 2), lax.rem(t, 3)
        return [
            remote(p_v.at[sl, sh_rows(2, 0, hs)], a1r.at[sl, 0], s_a1s.at[sl, 0], s_a1r.at[sl, 0], right),
            remote(p_v.at[sl, sh_rows(2, hs, hs)], a1r.at[sl, 1], s_a1s.at[sl, 1], s_a1r.at[sl, 1], left),
            remote(p_v.at[sl, sh_rows(1, hs, hs)], a2r.at[s3, 0], s_a2s.at[sl, 0], s_a2r.at[s3, 0], right),
            remote(p_v.at[sl, sh_rows(n_chip - 1, 0, hs)], a2r.at[s3, 1], s_a2s.at[sl, 1], s_a2r.at[s3, 1], left),
        ]

    def b_copies(t):
        sl = lax.rem(t, 2)
        return [
            remote(comb.at[sl, 0], br.at[sl, 0], s_bs.at[sl, 0], s_br.at[sl, 0], right),
            remote(comb.at[sl, 1], br.at[sl, 1], s_bs.at[sl, 1], s_br.at[sl, 1], left),
        ]

    def c_copies(t):
        sl = lax.rem(t, 2)
        rows = y_rows(t, 0, 0, shard)
        return [
            remote(ysh.at[sl], out.at[rows], s_cs.at[sl, 0], s_cr.at[sl, 0], right),
            remote(ysh.at[sl], out.at[rows], s_cs.at[sl, 1], s_cr.at[sl, 1], left),
        ]

    def y_local(t):
        sl = lax.rem(t, 2)
        return pltpu.make_async_copy(ysh.at[sl], out.at[y_rows(t, 0, 0, shard)], s_yl.at[sl])

    def d_copies(t):
        sl = lax.rem(t, 2)
        from_left = y_rows(t, n_chip - 1, 0, hs)
        from_right = y_rows(t, 1, hs, hs)
        return [
            remote(out.at[from_left], out.at[from_left], s_ds.at[sl, 0], s_dr.at[sl, 0], right),
            remote(out.at[from_right], out.at[from_right], s_ds.at[sl, 1], s_dr.at[sl, 1], left),
        ]

    def f_copy(t):
        rows = item_rows(t)
        return remote(out.at[rows], out.at[rows], s_f.at[0], s_f.at[1], mate)

    def phase_a(t):
        for c in a_copies(t):
            c.start()
        xres_load(t)

    def phase_b(t):
        sl = lax.rem(t, 2)

        @pl.when(t >= 2)
        def _():
            for c in b_copies(t - 2):
                c.wait_send()
        first = a_copies(t)
        first[0].wait_recv()
        first[1].wait_recv()
        comb[sl, 0] = (p_v[sl, sh_rows(1, 0, hs), :].astype(F32) + a1r[sl, 0].astype(F32)).astype(BF16)
        comb[sl, 1] = (p_v[sl, sh_rows(n_chip - 1, hs, hs), :].astype(F32) + a1r[sl, 1].astype(F32)).astype(BF16)
        for c in b_copies(t):
            c.start()

    def phase_c(t):
        sl, s3 = lax.rem(t, 2), lax.rem(t, 3)
        a = a_copies(t)
        b = b_copies(t)
        for c in a:
            c.wait_send()
        a[2].wait_recv()
        a[3].wait_recv()
        b[0].wait_recv()
        b[1].wait_recv()
        xres_wait(t)
        for k in range(2):
            rows = pl.ds(k * hs, hs)
            summed = p_v[sl, sh_rows(0, k * hs, hs), :].astype(F32) + br[sl, k].astype(F32) + a2r[s3, 1 - k].astype(F32)
            ysh[sl, rows, :] = (xres[sl, rows, :].astype(F32) + summed.astype(BF16).astype(F32)).astype(BF16)
        for c in c_copies(t):
            c.start()
        y_local(t).start()

    def phase_d(t):
        for c in c_copies(t):
            c.wait_recv()
        y_local(t).wait()
        for c in d_copies(t):
            c.start()

    def phase_e(t):
        for c in d_copies(t):
            c.wait_recv()
            c.wait_send()
        for c in c_copies(t):
            c.wait_send()

        @pl.when(t >= items)
        def _():
            f_copy(t).start()

    lane = lax.broadcasted_iota(jnp.int32, (ROWS, LANES), 1)

    def layer_norm(l):
        step = 64

        @pl.loop(0, ROWS // step)
        def _(i):
            r = pl.ds(pl.multiple_of(i * step, step), step)
            xf = x_v[r, :].astype(F32)
            mean = jnp.mean(xf, axis=-1, keepdims=True)
            centered = xf - mean
            var = jnp.mean(centered * centered, axis=-1, keepdims=True)
            n_v[r, :] = (centered * lax.rsqrt(var + LN_EPS) * gain[pl.ds(l, 1), :] + bias[pl.ds(l, 1), :]).astype(BF16)

    def qkv(blk):
        rows = pl.ds(pl.multiple_of(blk * ROWS, ROWS), ROWS)
        for g in range(2 * heads):
            y = jnp.dot(n_v[...], wq_v[g], preferred_element_type=F32)
            t0, t1 = y[:, :LANES], y[:, LANES:]
            cs, sn = cos_v[rows, :], sin_v[rows, :]
            for k, v in enumerate((t0 * cs - t1 * sn, t1 * cs + t0 * sn)):
                cols = pl.ds(k * LANES, LANES)
                q_v[g, :, cols] = jnp.where(lane < half_dim, v, 0.0).astype(BF16)
                kv_v[g, rows, cols] = pltpu.roll(v, LANES - half_dim, 1).astype(BF16)

    def attend(g, n):
        scores = lax.dot_general(q_v[g], kv_v[g, :n, :], (((1,), (1,)), ((), ())), preferred_element_type=F32)
        scores = scores * (head_dim ** -0.5 * np.log2(np.e))
        ri = lax.broadcasted_iota(jnp.int32, (ROWS, ROWS), 0)
        ci = lax.broadcasted_iota(jnp.int32, (ROWS, ROWS), 1)
        diag = jnp.where(ri >= ci, scores[:, n - ROWS:], -1e30)
        scores = jnp.concatenate([scores[:, :n - ROWS], diag], axis=1) if n > ROWS else diag
        e = jnp.exp2(scores - jnp.max(scores, axis=1, keepdims=True))
        probs = (e * (1.0 / jnp.sum(e, axis=1, keepdims=True))).astype(BF16)
        return jnp.dot(probs, kv_v[g, :n, :], preferred_element_type=F32)

    def attention(blk):
        for i in range(seq_blocks):
            @pl.when(blk == i)
            def _():
                n = (i + 1) * ROWS

                @pl.loop(0, 2)
                def _(h):
                    base = pl.multiple_of(h * ow, ow)
                    acc = [None, None]
                    for j in range(heads):
                        ctx = attend(h * heads + j, n)
                        for k in range(2):
                            c = ctx[:, k * LANES:(k + 1) * LANES]
                            if j == 0:
                                acc[k] = pltpu.roll(c, LANES - half_dim, 1)
                            elif j == 1:
                                acc[k] = jnp.where(lane < half_dim, acc[k], c)
                            elif j == 2:
                                c = pltpu.roll(c, half_dim, 1)
                                v = jnp.where(lane < 2 * half_dim, acc[k], jnp.where(lane < 3 * half_dim, c, 0.0))
                                cu_v[:, pl.ds(base + k * LANES, LANES)] = v.astype(BF16)
                            else:
                                v = jnp.where((lane >= half_dim) & (lane < 2 * half_dim), c, 0.0)
                                cu_v[:, pl.ds(base + (2 + k) * LANES, LANES)] = v.astype(BF16)

    def up():
        tile = 256
        for h in range(2):
            for n in range(ff // tile):
                y = jnp.dot(n_v[...], wu_v[h, :, n * tile:(n + 1) * tile], preferred_element_type=F32)
                u = 0.5 * y * (1.0 + lax.erf(y * np.float32(0.5 ** 0.5)))
                c = 2 * ow + h * ff + n * tile
                cu_v[:, c:c + tile] = u.astype(BF16)

    def down(t):
        tile = 256
        sl = lax.rem(t, 2)
        for n in range(d_model // tile):
            y = jnp.dot(cu_v[...], wod_v[:, n * tile:(n + 1) * tile], preferred_element_type=F32)
            p_v[sl, :, n * tile:(n + 1) * tile] = y.astype(BF16)

    barrier = pltpu.get_barrier_semaphore()
    for dev in (left, right, mate):
        pl.semaphore_signal(barrier, inc=1, device_id=dev, device_id_type=MESH)
    x_load(jnp.int32(0))
    for c in own_load(0):
        c.start()
    pl.semaphore_wait(barrier, 3)
    for c in push_first():
        c.start()

    @pl.loop(0, total + 4)
    def _(t):
        compute = t < total

        @pl.when(t == items)
        def _():
            for c in push_second():
                c.wait_recv()
            for c in own_load(1) + mate_load():
                c.start()

        @pl.when(compute)
        def _():
            x_wait()
            layer_norm(lax.div(t, items))

            @pl.when(t + 1 < total)
            def _():
                x_load(t + 1)

            blk = lax.rem(t, seq_blocks)
            wait_weights(t, [0])
            qkv(blk)
            attention(blk)
            wait_weights(t, [1])
            up()

        @pl.when(t == 2)
        def _():
            for c in push_second():
                c.start()

        @pl.when(t >= 4)
        def _():
            phase_e(t - 4)

        @pl.when((t >= 3) & (t < total + 3))
        def _():
            phase_d(t - 3)

        @pl.when((t >= 2) & (t < total + 2))
        def _():
            phase_c(t - 2)

        @pl.when(compute)
        def _():
            wait_weights(t, [2, 3])
            down(t)
            phase_a(t)

        @pl.when((t >= 1) & (t < total + 1))
        def _():
            phase_b(t - 1)

    for t in (total - 2, total - 1):
        for c in b_copies(jnp.int32(t)):
            c.wait_send()
    for c in push_first() + push_second():
        c.wait_send()
    half_rows = items * ROWS
    mine = out.at[pl.ds(pl.multiple_of(own_base, ROWS), half_rows)]
    every = remote(mine, mine, s_f.at[0], s_f.at[1], mate)
    every.wait_send()
    every.wait_recv()


def solution(mesh):
    n_tp = mesh.shape["tp"]
    n_chip = n_tp // CORES

    def shard_body(act_in, ln_gain, ln_bias, w_qkv, w_out, w_up, w_down):
        batch, seq_len, d_model = act_in.shape
        layers, _, heads, group_cols = w_qkv.shape
        head_dim = w_out.shape[1] // heads
        ff = w_up.shape[2]
        assert group_cols == 3 * head_dim and heads == 4 and head_dim == 2 * SLOT
        items = batch * seq_len // (CORES * ROWS)
        blocks = seq_len // ROWS
        cfg = (n_chip, layers, heads, head_dim, d_model, ff, items, blocks)
        shard = ROWS // n_chip
        ow = 4 * LANES
        w_q = prep_qkv(w_qkv, head_dim)
        w_o = prep_out(w_out, heads, head_dim)
        cos_tab, sin_tab = rope_tables(seq_len, head_dim)
        vm = pl.BlockSpec(memory_space=pltpu.VMEM)
        hb = pl.BlockSpec(memory_space=pl.ANY)
        dma = pltpu.SemaphoreType.DMA
        res = pl.pallas_call(
            functools.partial(body, cfg),
            name="layers",
            out_shape=[
                jax.ShapeDtypeStruct((batch * seq_len, d_model), BF16),
                jax.ShapeDtypeStruct((heads, d_model, 2 * LANES), BF16),
                jax.ShapeDtypeStruct((ow, d_model), BF16),
                jax.ShapeDtypeStruct((d_model, ff), BF16),
                jax.ShapeDtypeStruct((ff, d_model), BF16),
            ],
            in_specs=[hb] * 5 + [vm] * 4,
            out_specs=[hb] * 5,
            scratch_shapes=[
                pltpu.VMEM((ROWS, d_model), BF16),
                pltpu.VMEM((ROWS, d_model), BF16),
                pltpu.VMEM((2 * heads, ROWS, 2 * LANES), BF16),
                pltpu.VMEM((2 * heads, seq_len, 2 * LANES), BF16),
                pltpu.VMEM((ROWS, 2 * ow + 2 * ff), BF16),
                pltpu.VMEM((2, ROWS, d_model), BF16),
                pltpu.VMEM((2 * heads, d_model, 2 * LANES), BF16),
                pltpu.VMEM((2, d_model, ff), BF16),
                pltpu.VMEM((2 * ow + 2 * ff, d_model), BF16),
                pltpu.VMEM((2, 2, shard // 2, d_model), BF16),
                pltpu.VMEM((3, 2, shard // 2, d_model), BF16),
                pltpu.VMEM((2, 2, shard // 2, d_model), BF16),
                pltpu.VMEM((2, 2, shard // 2, d_model), BF16),
                pltpu.VMEM((2, shard, d_model), BF16),
                pltpu.VMEM((2, shard, d_model), BF16),
                dma((2, 2)), dma((2, 2)), dma((2, 2)), dma((3, 2)), dma((2, 2)), dma((2, 2)),
                dma((2, 2)), dma((2, 2)), dma((2, 2)), dma((2, 2)),
                dma((2,)), dma, dma((2,)), dma((2,)), dma((2, 4)), dma((2, 4)), dma((2, 4)),
            ],
            compiler_params=pltpu.CompilerParams(collective_id=0, has_side_effects=True, vmem_limit_bytes=VMEM_LIMIT),
        )(act_in.reshape(batch * seq_len, d_model), w_q, w_o, w_up, w_down, ln_gain, ln_bias, jnp.asarray(cos_tab), jnp.asarray(sin_tab))
        return res[0].reshape(batch, seq_len, d_model)

    return jax.shard_map(shard_body, mesh=mesh, in_specs=(P("dp", None, None), P(None, None), P(None, None), P(None, None, "tp", None), P(None, "tp", None), P(None, None, "tp"), P(None, "tp", None)), out_specs=P("dp", None, None), check_vma=False)
```

```python
import functools

import jax
import jax.numpy as jnp
import numpy as np
from jax import lax
from jax.experimental import pallas as pl
from jax.experimental.pallas import tpu as pltpu
from jax.sharding import PartitionSpec as P

LN_EPS = 1e-5
ROPE_BASE = 10000.0
F32 = jnp.float32
BF16 = jnp.bfloat16
MESH = pl.DeviceIdType.MESH
VMEM_LIMIT = 67043328

CORES = 2
ROWS = 256
LANES = 128
SLOT = 40


def rope_tables(seq_len, head_dim):
    half_dim = head_dim // 2
    inv_freq = (ROPE_BASE ** (-2.0 * np.arange(half_dim, dtype=np.float32) / head_dim)).astype(np.float32)
    angles = np.arange(seq_len, dtype=np.float32)[:, None] * inv_freq[None, :]
    cos_tab = np.ones((seq_len, LANES), np.float32)
    sin_tab = np.zeros((seq_len, LANES), np.float32)
    for k in range(2):
        cos_tab[:, k * half_dim:(k + 1) * half_dim] = np.cos(angles)
        sin_tab[:, k * half_dim:(k + 1) * half_dim] = np.sin(angles)
    return cos_tab, sin_tab


def regroup(head_dim):
    half_dim = head_dim // 2
    sel = np.zeros((3 * head_dim, 2 * LANES), np.float32)
    for part in range(3):
        for half in range(2):
            for i in range(half_dim):
                sel[(part * 2 + half) * half_dim + i, half * LANES + part * half_dim + i] = 1.0
    return sel


def body(cfg, act, w_q, w_o, w_u, w_d, gain, bias, cos_v, sin_v, sel_v,
         out, wu_v, wod_v, st_q, st_o, st_u, st_d, pq, po,
         stg, pst, pm, x_v, n_v, q_v, kv_v, cu_v, p_v, wq_v,
         a1r, a2r, br, comb, ysh, xres,
         s_a1s, s_a1r, s_a2s, s_a2r, s_bs, s_br, s_cs, s_cr, s_ds, s_dr, s_yl, s_x, s_xr, s_f, s_wl, s_ws, s_wr, s_stg, s_pm, s_pq, s_rl, s_fin):
    n_chip, layers, heads, head_dim, d_model, ff, items, blocks, late = cfg
    side_at = 3
    seq_blocks = blocks
    group_cols = 3 * head_dim
    half_dim = head_dim // 2
    total = layers * items
    tp = lax.axis_index("tp")
    chip = lax.div(tp, CORES)
    core = lax.rem(tp, CORES)
    right = {"tp": lax.rem(chip + 1, n_chip) * CORES + core}
    left = {"tp": lax.rem(chip + n_chip - 1, n_chip) * CORES + core}
    mate = {"tp": chip * CORES + (CORES - 1 - core)}
    own_base = core * (items * ROWS)
    mate_base = (CORES - 1 - core) * (items * ROWS)
    shard = ROWS // n_chip
    hs = shard // 2
    ow = 4 * LANES
    hw = ow + ff

    def ring(k):
        return lax.rem(chip + k, n_chip)

    def remote(src, dst, ssem, rsem, dev):
        return pltpu.make_async_remote_copy(src_ref=src, dst_ref=dst, send_sem=ssem, recv_sem=rsem, device_id=dev, device_id_type=MESH)

    def sh_rows(k, off, size):
        return pl.ds(pl.multiple_of(ring(k) * shard + off, hs), size)

    def y_rows(t, k, off, size):
        base = own_base + lax.rem(t, items) * ROWS
        return pl.ds(pl.multiple_of(base + ring(k) * shard + off, hs), size)

    def item_rows(t):
        return pl.ds(pl.multiple_of(own_base + lax.rem(t, items) * ROWS, ROWS), ROWS)

    def ud_dst(h):
        return [wu_v.at[:, pl.ds(h * ff, ff)], wod_v.at[pl.ds(h * hw + ow, ff)]]

    def own_ud(l):
        return [pltpu.make_async_copy(s.at[l], d, s_wl.at[0, i]) for i, (s, d) in enumerate(zip((w_u, w_d), ud_dst(0)))]

    def mate_ud():
        return [pltpu.make_async_copy(s, d, s_wl.at[1, i]) for i, (s, d) in enumerate(zip((st_u, st_d), ud_dst(1)))]

    def push(l, i):
        src = (w_q, w_o, w_u, w_d)[i].at[l]
        dst = (st_q.at[l], st_o.at[l], st_u if l else ud_dst(1)[0], st_d if l else ud_dst(1)[1])[i]
        return remote(src, dst, s_ws.at[l, i], s_wr.at[l, i], mate)

    def regroup_q(src, dst):
        for c in range(0, d_model, 512):
            y = lax.dot_general(src[:, c:c + 512], sel_v[...], (((0,), (0,)), ((), ())), preferred_element_type=F32)
            dst[c:c + 512, :] = y.astype(BF16)

    def regroup_o(src, dst):
        for c in range(0, d_model, 512):
            y = lax.dot_general(sel_v[...], src[:, c:c + 512], (((0,), (0,)), ((), ())), preferred_element_type=F32)
            dst[:, c:c + 512] = y.astype(BF16)

    slots = (stg.at[0], stg.at[1], cu_v.at[pl.ds(0, group_cols), pl.ds(0, d_model)])

    def q_copy(h, g):
        k = g % len(slots)
        return pltpu.make_async_copy((w_q, st_q)[h].at[0, g], slots[k], s_stg.at[k])

    def load_q(h):
        for g in range(heads):
            q_copy(0, g).wait()
            regroup_q(slots[g % len(slots)], wq_v.at[h * heads + g])
            if g + len(slots) < heads:
                @pl.when(h == 0)
                def _():
                    q_copy(0, g + len(slots)).start()

                @pl.when(h == 1)
                def _():
                    q_copy(1, g + len(slots)).start()

    def o_copy(l, h, k):
        rows = (pl.ds(0, group_cols), pl.ds(group_cols, head_dim))[k]
        return pltpu.make_async_copy((w_o, st_o)[h].at[l, rows], stg.at[k, pl.ds(0, (group_cols, head_dim)[k])], s_stg.at[k])

    def clear_tail():
        stg[1, head_dim:, :] = jnp.zeros((group_cols - head_dim, d_model), BF16)

    def start_o(h):
        clear_tail()

        @pl.when(h == 0)
        def _():
            for k in range(2):
                o_copy(0, 0, k).start()

        @pl.when(h == 1)
        def _():
            for k in range(2):
                o_copy(0, 1, k).start()

    def load_o(h):
        for k in range(2):
            o_copy(0, 0, k).wait()

        @pl.loop(0, 2)
        def _(k):
            regroup_o(stg.at[k], wod_v.at[pl.ds(pl.multiple_of(h * hw + k * 2 * LANES, 2 * LANES), 2 * LANES)])

    n_side = 2 * heads + 4

    def side_copy(a):
        for h in range(2):
            @pl.when((a >= h * heads) & (a < (h + 1) * heads))
            def _():
                sl = lax.rem(a, 2)
                pltpu.make_async_copy((w_q, st_q)[h].at[1, a - h * heads], stg.at[sl], s_stg.at[sl]).start()

            for k in range(2):
                @pl.when(a == 2 * heads + 2 * h + k)
                def _():
                    o_copy(1, h, k).start()

    def pq_copy(g):
        return pltpu.make_async_copy(pst, pq.at[g], s_pq.at[0])

    def po_copy(b):
        return pltpu.make_async_copy(pm, po.at[pl.ds(pl.multiple_of(b * 2 * LANES, 2 * LANES), 2 * LANES)], s_pq.at[1])

    def side_job(a):
        sl = lax.rem(a, 2)

        @pl.when(a == heads - 1)
        def _():
            push(1, 0).wait_recv()

        @pl.when(a == 2 * heads + 1)
        def _():
            push(1, 1).wait_recv()

        @pl.when(a < 2 * heads)
        def _():
            pltpu.make_async_copy(w_q.at[1, 0], stg.at[sl], s_stg.at[sl]).wait()

            @pl.when(a > 0)
            def _():
                pq_copy(a - 1).wait()

            regroup_q(stg.at[sl], pst)
            pq_copy(a).start()

        @pl.when(a >= 2 * heads)
        def _():
            for k in range(2):
                @pl.when(sl == k)
                def _():
                    o_copy(1, 0, k).wait()

            @pl.when(a > 2 * heads)
            def _():
                po_copy(a - 2 * heads - 1).wait()

            regroup_o(stg.at[sl], pm)
            po_copy(a - 2 * heads).start()

        @pl.when(a == 2 * heads)
        def _():
            clear_tail()

        @pl.when(a + 1 < n_side)
        def _():
            side_copy(a + 1)

    def load_second(k):
        if k == 0:
            return [pltpu.make_async_copy(pq, wq_v, s_rl.at[0])]
        if k == 1:
            return [own_ud(1)[0], mate_ud()[0]]
        outs = [pltpu.make_async_copy(po.at[pl.ds(h * ow, ow)], wod_v.at[pl.ds(h * hw, ow)], s_rl.at[1 + h]) for h in range(2)]
        return [own_ud(1)[1], mate_ud()[1]] + outs

    def wait_ud(i, k):
        @pl.when(i == 0)
        def _():
            own_ud(0)[k].wait()

        @pl.when(i == 2)
        def _():
            push(0, 2 + k).wait_recv()

        @pl.when(i == items + 1)
        def _():
            for c in load_second(1 + k):
                c.wait()

    def x_load(i):
        t = i - 1

        @pl.when(i == 0)
        def _():
            pltpu.make_async_copy(act.at[pl.ds(pl.multiple_of(mate_base, ROWS), ROWS)], x_v, s_x).start()

        @pl.when((i >= 1) & (t < items))
        def _():
            pltpu.make_async_copy(act.at[item_rows(t)], x_v, s_x).start()

        @pl.when(t >= items)
        def _():
            pltpu.make_async_copy(out.at[item_rows(t)], x_v, s_x).start()

    def x_wait():
        pltpu.make_async_copy(act.at[pl.ds(0, ROWS)], x_v, s_x).wait()

    def xres_load(t):
        sl = lax.rem(t, 2)

        @pl.when(t < items)
        def _():
            pltpu.make_async_copy(act.at[y_rows(t, 0, 0, shard)], xres.at[sl], s_xr.at[sl]).start()

        @pl.when(t >= items)
        def _():
            pltpu.make_async_copy(out.at[y_rows(t, 0, 0, shard)], xres.at[sl], s_xr.at[sl]).start()

    def xres_wait(t):
        sl = lax.rem(t, 2)
        pltpu.make_async_copy(act.at[pl.ds(0, shard)], xres.at[sl], s_xr.at[sl]).wait()

    def a_copies(t):
        sl = lax.rem(t, 2)
        return [
            remote(p_v.at[sh_rows(2, 0, hs)], a1r.at[sl, 0], s_a1s.at[sl, 0], s_a1r.at[sl, 0], right),
            remote(p_v.at[sh_rows(2, hs, hs)], a1r.at[sl, 1], s_a1s.at[sl, 1], s_a1r.at[sl, 1], left),
            remote(p_v.at[sh_rows(1, hs, hs)], a2r.at[sl, 0], s_a2s.at[sl, 0], s_a2r.at[sl, 0], right),
            remote(p_v.at[sh_rows(n_chip - 1, 0, hs)], a2r.at[sl, 1], s_a2s.at[sl, 1], s_a2r.at[sl, 1], left),
        ]

    def b_copies(t):
        sl = lax.rem(t, 2)
        return [
            remote(comb.at[sl, 0], br.at[sl, 0], s_bs.at[sl, 0], s_br.at[sl, 0], right),
            remote(comb.at[sl, 1], br.at[sl, 1], s_bs.at[sl, 1], s_br.at[sl, 1], left),
        ]

    def c_copies(t):
        sl = lax.rem(t, 2)
        rows = y_rows(t, 0, 0, shard)
        return [
            remote(ysh.at[sl], out.at[rows], s_cs.at[sl, 0], s_cr.at[sl, 0], right),
            remote(ysh.at[sl], out.at[rows], s_cs.at[sl, 1], s_cr.at[sl, 1], left),
        ]

    def y_local(t):
        sl = lax.rem(t, 2)
        return pltpu.make_async_copy(ysh.at[sl], out.at[y_rows(t, 0, 0, shard)], s_yl.at[sl])

    def d_copies(t):
        sl = lax.rem(t, 2)
        from_left = y_rows(t, n_chip - 1, 0, hs)
        from_right = y_rows(t, 1, hs, hs)
        return [
            remote(out.at[from_left], out.at[from_left], s_ds.at[sl, 0], s_dr.at[sl, 0], right),
            remote(out.at[from_right], out.at[from_right], s_ds.at[sl, 1], s_dr.at[sl, 1], left),
        ]

    def f_copy(t, group):
        rows = item_rows(t)
        return remote(out.at[rows], out.at[rows], s_f.at[0, group], s_f.at[1, group], mate)

    def phase_a(t):
        for c in a_copies(t):
            c.start()
        xres_load(t)

    def phase_b(t):
        sl = lax.rem(t, 2)

        @pl.when(t >= 2)
        def _():
            for c in b_copies(t - 2):
                c.wait_send()
        first = a_copies(t)
        first[0].wait_recv()
        first[1].wait_recv()
        comb[sl, 0] = (p_v[sh_rows(1, 0, hs), :].astype(F32) + a1r[sl, 0].astype(F32)).astype(BF16)
        comb[sl, 1] = (p_v[sh_rows(n_chip - 1, hs, hs), :].astype(F32) + a1r[sl, 1].astype(F32)).astype(BF16)
        for c in b_copies(t):
            c.start()

    def phase_c(t):
        sl = lax.rem(t, 2)
        a = a_copies(t)
        b = b_copies(t)
        for c in a:
            c.wait_send()
        a[2].wait_recv()
        a[3].wait_recv()
        b[0].wait_recv()
        b[1].wait_recv()
        xres_wait(t)
        for k in range(2):
            rows = pl.ds(k * hs, hs)
            summed = p_v[sh_rows(0, k * hs, hs), :].astype(F32) + br[sl, k].astype(F32) + a2r[sl, 1 - k].astype(F32)
            ysh[sl, rows, :] = (xres[sl, rows, :].astype(F32) + summed.astype(BF16).astype(F32)).astype(BF16)
        for c in c_copies(t):
            c.start()
        y_local(t).start()

    def phase_d(t):
        for c in c_copies(t):
            c.wait_recv()
        y_local(t).wait()
        for c in d_copies(t):
            c.start()

    def phase_e(t):
        for c in d_copies(t):
            c.wait_recv()
            c.wait_send()
        for c in c_copies(t):
            c.wait_send()

        @pl.when((t >= items) & (t < total - late))
        def _():
            f_copy(t, 0).start()

        @pl.when(t >= total - late)
        def _():
            f_copy(t, 1).start()

    lane = lax.broadcasted_iota(jnp.int32, (ROWS, LANES), 1)

    def layer_norm(l):
        xf = x_v[...].astype(F32)
        mean = jnp.mean(xf, axis=-1, keepdims=True)
        centered = xf - mean
        var = jnp.mean(centered * centered, axis=-1, keepdims=True)
        n_v[...] = (centered * lax.rsqrt(var + LN_EPS) * gain[pl.ds(l, 1), :] + bias[pl.ds(l, 1), :]).astype(BF16)

    def qkv(blk, h):
        rows = pl.ds(pl.multiple_of(blk * ROWS, ROWS), ROWS)
        for j in range(heads):
            g = h * heads + j
            y = jnp.dot(n_v[...], wq_v[g], preferred_element_type=F32)
            t0, t1 = y[:, :LANES], y[:, LANES:]
            cs, sn = cos_v[rows, :], sin_v[rows, :]
            for k, v in enumerate((t0 * cs - t1 * sn, t1 * cs + t0 * sn)):
                cols = pl.ds(k * LANES, LANES)
                q_v[g, :, cols] = jnp.where(lane < half_dim, v, 0.0).astype(BF16)
                kv_v[g, rows, cols] = pltpu.roll(v, LANES - half_dim, 1).astype(BF16)

    def attend(g, n):
        scores = lax.dot_general(q_v[g], kv_v[g, :n, :], (((1,), (1,)), ((), ())), preferred_element_type=F32)
        scores = scores * (head_dim ** -0.5 * np.log2(np.e))
        ri = lax.broadcasted_iota(jnp.int32, (ROWS, ROWS), 0)
        ci = lax.broadcasted_iota(jnp.int32, (ROWS, ROWS), 1)
        diag = jnp.where(ri >= ci, scores[:, n - ROWS:], -1e30)
        scores = jnp.concatenate([scores[:, :n - ROWS], diag], axis=1) if n > ROWS else diag
        e = jnp.exp2(scores - jnp.max(scores, axis=1, keepdims=True))
        probs = (e * (1.0 / jnp.sum(e, axis=1, keepdims=True))).astype(BF16)
        return jnp.dot(probs, kv_v[g, :n, :], preferred_element_type=F32)

    def attention(blk, halves):
        for i in range(seq_blocks):
            @pl.when(blk == i)
            def _():
                n = (i + 1) * ROWS

                @pl.loop(0, halves)
                def _(h):
                    base = pl.multiple_of(h * hw, 2 * LANES)
                    acc = [None, None]
                    for j in range(heads):
                        ctx = attend(h * heads + j, n)
                        for k in range(2):
                            c = ctx[:, k * LANES:(k + 1) * LANES]
                            if j == 0:
                                acc[k] = pltpu.roll(c, LANES - half_dim, 1)
                            elif j == 1:
                                acc[k] = jnp.where(lane < half_dim, acc[k], c)
                            elif j == 2:
                                c = pltpu.roll(c, half_dim, 1)
                                v = jnp.where(lane < 2 * half_dim, acc[k], jnp.where(lane < 3 * half_dim, c, 0.0))
                                cu_v[:, pl.ds(base + k * LANES, LANES)] = v.astype(BF16)
                            else:
                                v = jnp.where(lane < half_dim, pltpu.roll(c, LANES - half_dim, 1), 0.0)
                                cu_v[:, pl.ds(base + (2 + k) * LANES, LANES)] = v.astype(BF16)

    def up(h):
        tile = 256
        for n in range(ff // tile):
            y = jnp.dot(n_v[...], wu_v[:, pl.ds(pl.multiple_of(h * ff + n * tile, tile), tile)], preferred_element_type=F32)
            u = 0.5 * y * (1.0 + lax.erf(y * np.float32(0.5 ** 0.5)))
            cu_v[:, pl.ds(pl.multiple_of(h * hw + ow + n * tile, tile), tile)] = u.astype(BF16)

    def down(depth):
        tile = 256
        for n in range(d_model // tile):
            y = jnp.dot(cu_v[:, :depth], wod_v[:depth, n * tile:(n + 1) * tile], preferred_element_type=F32)
            p_v[:, n * tile:(n + 1) * tile] = y.astype(BF16)

    def pm_copy():
        return remote(p_v, pm, s_pm.at[0], s_pm.at[1], mate)

    def f_wait(first, count, group):
        rows = out.at[pl.ds(pl.multiple_of(own_base + first * ROWS, ROWS), count * ROWS)]
        both = remote(rows, rows, s_f.at[0, group], s_f.at[1, group], mate)
        both.wait_send()
        both.wait_recv()

    own_a, mate_a, own_b = final_split(items, late, d_model, 2 * hw)

    def final_load(k):
        def rows(base, first, count):
            return out.at[pl.ds(pl.multiple_of(base + first * ROWS, ROWS), count * ROWS)]

        if k == 0:
            return pltpu.make_async_copy(rows(own_base, 0, own_a), wu_v.at[pl.ds(0, own_a * ROWS)], s_fin.at[0])
        if k == 1:
            return pltpu.make_async_copy(rows(mate_base, 0, mate_a), wod_v.at[pl.ds(0, mate_a * ROWS)], s_fin.at[1])
        return pltpu.make_async_copy(rows(own_base, own_a, own_b), wod_v.at[pl.ds(mate_a * ROWS, own_b * ROWS)], s_fin.at[2])

    barrier = pltpu.get_barrier_semaphore()
    for dev in (left, right, mate):
        pl.semaphore_signal(barrier, inc=1, device_id=dev, device_id_type=MESH)
    x_load(jnp.int32(0))
    for g in range(len(slots)):
        q_copy(0, g).start()
    pl.semaphore_wait(barrier, 3)
    for k in range(2):
        push(0, k).start()

    @pl.loop(0, total + 4)
    def _(i):
        t = i - 1
        tc = jnp.maximum(t, 0)
        compute = i <= total
        blk = lax.rem(tc, seq_blocks)
        halves = jnp.where(i < 2, 1, 2)

        @pl.when((i == 0) | (i == 2))
        def _():
            h = lax.div(i, 2)
            load_q(h)

            @pl.when(i == 0)
            def _():
                for c in own_ud(0):
                    c.start()

            @pl.when(i == 2)
            def _():
                push(0, 1).wait_recv()

            start_o(h)

            @pl.when(i == 2)
            def _():
                qkv(jnp.int32(0), 1)

        @pl.when(compute)
        def _():
            x_wait()
            layer_norm(lax.div(tc, items))

            @pl.when(i < total)
            def _():
                x_load(i + 1)

        @pl.when(t == 1)
        def _():
            phase_b(t - 1)

        @pl.when(t == items)
        def _():
            for c in load_second(0):
                c.wait()

        @pl.when(compute)
        def _():
            @pl.loop(0, halves)
            def _(h):
                qkv(blk, h)

        @pl.when((t >= 2) & (t < total + 1))
        def _():
            phase_b(t - 1)

        @pl.when(t == items - 1)
        def _():
            pq_copy(0).wait()
            po_copy(0).wait()
            for c in load_second(0):
                c.start()

        @pl.when(compute)
        def _():
            attention(blk, halves)

        @pl.when((t >= side_at) & (t < side_at + n_side))
        def _():
            side_job(t - side_at)

        @pl.when((t >= 2) & (t < total + 2))
        def _():
            phase_d(t - 2)

        @pl.when(t >= 3)
        def _():
            phase_e(t - 3)

        @pl.when(compute)
        def _():
            wait_ud(i, 0)

            @pl.loop(0, halves)
            def _(h):
                up(h)

        @pl.when(t == items - 1)
        def _():
            for k in range(2, 4):
                push(1, k).wait_recv()
            for c in load_second(1):
                c.start()

        @pl.when(t == total - 1)
        def _():
            final_load(0).start()

        @pl.when((t >= 1) & (t < total + 1))
        def _():
            phase_c(t - 1)

        @pl.when((i == 0) | (i == 2))
        def _():
            load_o(lax.div(i, 2))

        @pl.when(i < 2)
        def _():
            @pl.when(i == 1)
            def _():
                pm_copy().wait_send()

            wait_ud(i, 1)
            down(hw)

            @pl.when(i == 0)
            def _():
                pm_copy().start()
                for k in range(2, 4):
                    push(0, k).start()

            @pl.when(i == 1)
            def _():
                pm_copy().wait_recv()
                p_v[...] = (p_v[...].astype(F32) + pm[...].astype(F32)).astype(BF16)
                phase_a(t)
                push(0, 0).wait_recv()
                for g in range(len(slots)):
                    q_copy(1, g).start()

        @pl.when((i >= 2) & compute)
        def _():
            wait_ud(i, 1)
            down(2 * hw)
            phase_a(t)

        @pl.when(t == items - 1)
        def _():
            for c in load_second(2):
                c.start()

        @pl.when(t == total - 1)
        def _():
            f_wait(0, mate_a, 0)
            for k in (1, 2):
                final_load(k).start()

        @pl.when(t == 2)
        def _():
            for k in range(4):
                push(1, k).start()

        @pl.when(t == side_at - 1)
        def _():
            side_copy(jnp.int32(0))

    for t in (total - 2, total - 1):
        for c in b_copies(jnp.int32(t)):
            c.wait_send()
    for l in range(layers):
        for i in range(4):
            push(l, i).wait_send()
    f_wait(mate_a, late, 1)
    for k in range(3):
        final_load(k).wait()


def final_split(items, late, rows_a, rows_b):
    own_a = rows_a // ROWS
    mate_a = items - late
    return own_a, mate_a, rows_b // ROWS - mate_a


def collect(cfg, y, va, vb, out, buf, sem):
    items, late = cfg
    core = lax.rem(lax.axis_index("tp"), CORES)
    own_base = core * (items * ROWS)
    mate_base = (CORES - 1 - core) * (items * ROWS)
    own_a, mate_a, own_b = final_split(items, late, va.shape[0], vb.shape[0])

    def rows(base, first, count):
        return pl.ds(pl.multiple_of(base + first * ROWS, ROWS), count * ROWS)

    rest = [(own_base, k) for k in range(own_a + own_b, items)] + [(mate_base, k) for k in range(mate_a, items)]
    ins = [pltpu.make_async_copy(y.at[rows(b, k, 1)], buf.at[n], sem.at[3 + n]) for n, (b, k) in enumerate(rest)]
    outs = [pltpu.make_async_copy(buf.at[n], out.at[rows(b, k, 1)], sem.at[3 + n]) for n, (b, k) in enumerate(rest)]
    direct = [
        pltpu.make_async_copy(va, out.at[rows(own_base, 0, own_a)], sem.at[0]),
        pltpu.make_async_copy(vb.at[pl.ds(0, mate_a * ROWS)], out.at[rows(mate_base, 0, mate_a)], sem.at[1]),
        pltpu.make_async_copy(vb.at[pl.ds(mate_a * ROWS, own_b * ROWS)], out.at[rows(own_base, own_a, own_b)], sem.at[2]),
    ]
    for c in ins + direct:
        c.start()
    for c, d in zip(ins, outs):
        c.wait()
        d.start()
    for c in direct + outs:
        c.wait()


def solution(mesh):
    n_tp = mesh.shape["tp"]
    n_chip = n_tp // CORES

    def shard_body(act_in, ln_gain, ln_bias, w_qkv, w_out, w_up, w_down):
        batch, seq_len, d_model = act_in.shape
        layers, _, heads, group_cols = w_qkv.shape
        head_dim = w_out.shape[1] // heads
        ff = w_up.shape[2]
        assert group_cols == 3 * head_dim and heads == 4 and head_dim == 2 * SLOT
        items = batch * seq_len // (CORES * ROWS)
        blocks = seq_len // ROWS
        late = 4
        cfg = (n_chip, layers, heads, head_dim, d_model, ff, items, blocks, late)
        shard = ROWS // n_chip
        ow = 4 * LANES
        w_q = jnp.transpose(w_qkv, (0, 2, 3, 1))
        cos_tab, sin_tab = rope_tables(seq_len, head_dim)
        vm = pl.BlockSpec(memory_space=pltpu.VMEM)
        hb = pl.BlockSpec(memory_space=pl.ANY)
        dma = pltpu.SemaphoreType.DMA
        out_vmem = (d_model * 2 * ff + (2 * ow + 2 * ff) * d_model) * 2
        res = pl.pallas_call(
            functools.partial(body, cfg),
            name="layers",
            out_shape=[
                jax.ShapeDtypeStruct((batch * seq_len, d_model), BF16),
                pltpu.VMEM((d_model, 2 * ff), BF16),
                pltpu.VMEM((2 * ow + 2 * ff, d_model), BF16),
                jax.ShapeDtypeStruct((layers, heads, group_cols, d_model), BF16),
                jax.ShapeDtypeStruct((layers, heads * head_dim, d_model), BF16),
                jax.ShapeDtypeStruct((d_model, ff), BF16),
                jax.ShapeDtypeStruct((ff, d_model), BF16),
                jax.ShapeDtypeStruct((2 * heads, d_model, 2 * LANES), BF16),
                jax.ShapeDtypeStruct((2 * ow, d_model), BF16),
            ],
            in_specs=[hb] * 5 + [vm] * 5,
            out_specs=[hb, vm, vm] + [hb] * 6,
            scratch_shapes=[
                pltpu.VMEM((2, group_cols, d_model), BF16),
                pltpu.VMEM((d_model, 2 * LANES), BF16),
                pltpu.VMEM((ROWS, d_model), BF16),
                pltpu.VMEM((ROWS, d_model), BF16),
                pltpu.VMEM((ROWS, d_model), BF16),
                pltpu.VMEM((2 * heads, ROWS, 2 * LANES), BF16),
                pltpu.VMEM((2 * heads, seq_len, 2 * LANES), BF16),
                pltpu.VMEM((ROWS, 2 * ow + 2 * ff), BF16),
                pltpu.VMEM((ROWS, d_model), BF16),
                pltpu.VMEM((2 * heads, d_model, 2 * LANES), BF16),
                pltpu.VMEM((2, 2, shard // 2, d_model), BF16),
                pltpu.VMEM((2, 2, shard // 2, d_model), BF16),
                pltpu.VMEM((2, 2, shard // 2, d_model), BF16),
                pltpu.VMEM((2, 2, shard // 2, d_model), BF16),
                pltpu.VMEM((2, shard, d_model), BF16),
                pltpu.VMEM((2, shard, d_model), BF16),
                dma((2, 2)), dma((2, 2)), dma((2, 2)), dma((2, 2)), dma((2, 2)), dma((2, 2)),
                dma((2, 2)), dma((2, 2)), dma((2, 2)), dma((2, 2)),
                dma((2,)), dma, dma((2,)), dma((2, 2)), dma((2, 2)), dma((2, 4)), dma((2, 4)), dma((3,)), dma((2,)),
                dma((2,)), dma((3,)), dma((3,)),
            ],
            compiler_params=pltpu.CompilerParams(collective_id=0, has_side_effects=True, vmem_limit_bytes=VMEM_LIMIT - out_vmem),
        )(act_in.reshape(batch * seq_len, d_model), w_q, w_out, w_up, w_down, ln_gain, ln_bias, jnp.asarray(cos_tab), jnp.asarray(sin_tab), jnp.asarray(regroup(head_dim), BF16))
        own_a, mate_a, own_b = final_split(items, late, d_model, 2 * ow + 2 * ff)
        rest = 2 * items - own_a - mate_a - own_b
        y = pl.pallas_call(
            functools.partial(collect, (items, late)),
            name="collect",
            out_shape=jax.ShapeDtypeStruct((batch * seq_len, d_model), BF16),
            in_specs=[hb, vm, vm],
            out_specs=hb,
            scratch_shapes=[pltpu.VMEM((rest, ROWS, d_model), BF16), dma((3 + rest,))],
            compiler_params=pltpu.CompilerParams(vmem_limit_bytes=16 << 20),
        )(*res[:3])
        return y.reshape(batch, seq_len, d_model)

    return jax.shard_map(shard_body, mesh=mesh, in_specs=(P("dp", None, None), P(None, None), P(None, None), P(None, None, "tp", None), P(None, "tp", None), P(None, None, "tp"), P(None, "tp", None)), out_specs=P("dp", None, None), check_vma=False)
```

```python
import functools

import jax
import jax.numpy as jnp
import numpy as np
from jax import lax
from jax.experimental import pallas as pl
from jax.experimental.pallas import tpu as pltpu
from jax.sharding import PartitionSpec as P

LN_EPS = 1e-5
ROPE_BASE = 10000.0
F32 = jnp.float32
BF16 = jnp.bfloat16
MESH = pl.DeviceIdType.MESH
VMEM_LIMIT = 67043328

CORES = 2
ROWS = 256
LANES = 128
SLOT = 40
LN_ROWS = 128
UNROLLED = 3


def rope_tables(seq_len, head_dim):
    half_dim = head_dim // 2
    inv_freq = (ROPE_BASE ** (-2.0 * np.arange(half_dim, dtype=np.float32) / head_dim)).astype(np.float32)
    angles = np.arange(seq_len, dtype=np.float32)[:, None] * inv_freq[None, :]
    cos_tab = np.ones((seq_len, LANES), np.float32)
    sin_tab = np.zeros((seq_len, LANES), np.float32)
    for k in range(2):
        cos_tab[:, k * half_dim:(k + 1) * half_dim] = np.cos(angles)
        sin_tab[:, k * half_dim:(k + 1) * half_dim] = np.sin(angles)
    return np.concatenate([cos_tab, sin_tab], axis=1)


def regroup(head_dim):
    half_dim = head_dim // 2
    sel = np.zeros((3 * head_dim, 2 * LANES), np.float32)
    for part in range(3):
        for half in range(2):
            for i in range(half_dim):
                sel[(part * 2 + half) * half_dim + i, half * LANES + part * half_dim + i] = 1.0
    return sel


def body(cfg, act, w_q, w_o, w_u, w_d, gain, bias, tab, sel_v,
         out, wu_v, wod_v, st_q, st_o, st_u, st_d, pq, po,
         tab_v, pst, pm, x_v, n_v, q_v, kv_v, cu_v, p_v, wq_v,
         ar, br, ysh, br2, ysh2,
         s_as, s_ar, s_ar2, s_bs, s_br, s_br2, s_cs, s_cr, s_co, s_ds, s_do, s_y1, s_yl, s_x, s_xr, s_f, s_wl, s_ws, s_wr, s_m2s, s_m2r,
         s_gs, s_gx, s_gp, s_stg, s_pm, s_pq, s_rl, s_fin, s_tab, s_kv, s_ca, s_cb, s_rdy):
    n_chip, layers, heads, head_dim, d_model, ff, items, blocks, late = cfg
    side_at = 9
    group_cols = 3 * head_dim
    seq_blocks = blocks
    group_cols = 3 * head_dim
    half_dim = head_dim // 2
    total = layers * items
    tp = lax.axis_index("tp")
    dp = lax.axis_index("dp")
    chip = lax.div(tp, CORES)
    core = lax.rem(tp, CORES)
    twin = lax.rem(dp, 2)
    odd = lax.rem(chip, 2)
    pair = lax.div(chip, 2)
    inn = chip + 1 - 2 * odd
    outn = lax.rem(chip + n_chip - 1 + 2 * odd, n_chip)

    def dev(c, k):
        return {"tp": c * CORES + k}

    inn_d, outn_d, mate = dev(inn, core), dev(outn, core), dev(chip, CORES - 1 - core)
    peer = {"dp": dp + 1 - 2 * twin, "tp": tp}
    own_base = core * (items * ROWS)
    mate_base = (CORES - 1 - core) * (items * ROWS)
    half = ROWS // 2
    quart = ROWS // 4
    ow = 4 * LANES
    hw = ow + ff

    def remote(src, dst, ssem, rsem, dev):
        return pltpu.make_async_remote_copy(src_ref=src, dst_ref=dst, send_sem=ssem, recv_sem=rsem, device_id=dev, device_id_type=MESH)

    def at(base, off, size):
        return pl.ds(pl.multiple_of(base + off, quart), size)

    def rows1(t, off, size):
        return at(own_base + lax.rem(t, items) * ROWS, off, size)

    def rows2(t, p, off, size):
        u = t - items
        q = lax.div(u, blocks)
        cc = lax.rem(q, CORES)
        seq = p + cc - 2 * p * cc + 2 * lax.div(q, CORES)
        return at(cc * (items * ROWS) + (seq * blocks + lax.rem(u, blocks)) * ROWS, off, size)

    def owner(t):
        return lax.rem(lax.div(t, blocks) + core, 2) == pair

    def ud_dst(h):
        return [wu_v.at[:, pl.ds(h * ff, ff)], wod_v.at[pl.ds(h * hw + ow, ff)]]

    def own_ud(l):
        return [pltpu.make_async_copy(s.at[l], d, s_wl.at[0, i]) for i, (s, d) in enumerate(zip((w_u, w_d), ud_dst(0)))]

    def staged_ud(h):
        return [pltpu.make_async_copy(s.at[h], d, s_wl.at[h, i]) for i, (s, d) in enumerate(zip((st_u, st_d), ud_dst(h)))]

    def push(i):
        src = (wq_v.at[pl.ds(0, heads)], wod_v.at[pl.ds(0, ow)], w_u.at[0], w_d.at[0])[i]
        dst = (wq_v.at[pl.ds(heads, heads)], wod_v.at[pl.ds(hw, ow)], *ud_dst(1))[i]
        return remote(src, dst, s_ws.at[i], s_wr.at[i], mate)

    def push_kv():
        rows = pl.ds(0, ROWS)
        return remote(kv_v.at[pl.ds(0, heads), rows], kv_v.at[pl.ds(heads, heads), rows], s_kv.at[0], s_kv.at[1], mate)

    args2 = (w_q.at[1], w_o.at[1], w_u.at[1], w_d.at[1])
    staged = (st_q, st_o, st_u, st_d)

    def push2(i):
        return remote(args2[i], staged[i].at[1], s_m2s.at[i], s_m2r.at[i], mate)

    pieces = []
    for k, (n_rows, step) in enumerate(((heads * group_cols, quart), (heads * head_dim, quart), (d_model, 2 * quart), (ff, quart))):
        pieces += [(k, r, step) for r in range(0, n_rows, step)]
    groups = [pieces[j:j + 4] for j in range(0, len(pieces), 4)]

    def group_send(j, k):
        arr, r, n = groups[j][k]
        rows = pl.ds(r, n)
        return remote(args2[arr].at[rows], staged[arr].at[twin, rows], s_gs.at[0], s_gx.at[j], dev(outn, 1))

    def group_pass(j):
        copies = []
        for arr in range(4):
            mine = [p for p in groups[j] if p[0] == arr]
            if mine:
                rows = pl.ds(mine[0][1], sum(p[2] for p in mine))
                copies.append(remote(staged[arr].at[twin, rows], staged[arr].at[twin, rows], s_gs.at[1], s_gp.at[j], peer))
        return copies

    def group_bytes(j, sem, n=1):
        rows = out.at[pl.ds(0, n * ROWS)]
        return remote(rows, rows, s_gs.at[j], sem, peer)

    def regroup_q(src, dst, unroll=False):
        def one(c):
            part = pl.ds(c, 512) if unroll else pl.ds(pl.multiple_of(c, 512), 512)
            y = lax.dot_general(src[:, part], sel_v[...], (((0,), (0,)), ((), ())), preferred_element_type=F32)
            dst[part, :] = y.astype(BF16)

        if unroll:
            for c in range(0, d_model, 512):
                one(c)
        else:
            pl.loop(0, d_model, step=512)(one)

    def regroup_o(src, dst):
        @pl.loop(0, d_model, step=512)
        def _(c):
            part = pl.ds(pl.multiple_of(c, 512), 512)
            y = lax.dot_general(sel_v[...], src[:, part], (((0,), (0,)), ((), ())), preferred_element_type=F32)
            dst[:, part] = y.astype(BF16)

    slots = (p_v.at[1, pl.ds(0, group_cols)], p_v.at[2, pl.ds(0, group_cols)], cu_v.at[pl.ds(0, group_cols), pl.ds(0, d_model)])

    def q_copy(g):
        return pltpu.make_async_copy(w_q.at[0, pl.ds(g * group_cols, group_cols)], slots[g % len(slots)], s_stg.at[g % len(slots)])

    def load_q():
        for g in range(heads):
            q_copy(g).wait()
            regroup_q(slots[g % len(slots)], wq_v.at[g])
            if g + len(slots) < heads:
                q_copy(g + len(slots)).start()

    def o_copy(src, k, dst):
        rows = (pl.ds(0, group_cols), pl.ds(group_cols, head_dim))[k]
        return pltpu.make_async_copy(src.at[rows], dst.at[pl.ds(0, (group_cols, head_dim)[k])], s_stg.at[k])

    def clear_tail(ref):
        ref[pl.ds(head_dim, group_cols - head_dim), :] = jnp.zeros((group_cols - head_dim, d_model), BF16)

    def load_o():
        for k in range(2):
            o_copy(w_o.at[0], k, slots[k]).wait()
            regroup_o(slots[k], wod_v.at[pl.ds(k * 2 * LANES, 2 * LANES)])

    n_side = 2 * heads + 4
    side_refs = (n_v.at[pl.ds(0, group_cols)], slots[2])

    def side_copy(a, k):
        for h in range(2):
            for arg in range(2 - h):
                from_arg = (core == 0) if arg else ((core == 1) if h == 0 else (core >= 0))

                @pl.when((a >= h * heads) & (a < (h + 1) * heads) & from_arg)
                def _():
                    rows = pl.ds(pl.multiple_of((a - h * heads) * group_cols, group_cols), group_cols)
                    src = w_q.at[1, rows] if arg else st_q.at[h, rows]
                    pltpu.make_async_copy(src, side_refs[k], s_stg.at[k]).start()

                @pl.when((a == 2 * heads + 2 * h + k) & from_arg)
                def _():
                    if k:
                        clear_tail(side_refs[k])
                    o_copy(w_o.at[1] if arg else st_o.at[h], k, side_refs[k]).start()

    def pq_copy(g):
        return pltpu.make_async_copy(pst, pq.at[g], s_pq.at[0])

    def po_copy(b):
        return pltpu.make_async_copy(pm, po.at[pl.ds(pl.multiple_of(b * 2 * LANES, 2 * LANES), 2 * LANES)], s_pq.at[1])

    def side_job(a, k):
        @pl.when(a < 2 * heads)
        def _():
            pltpu.make_async_copy(w_q.at[1, pl.ds(0, group_cols)], side_refs[k], s_stg.at[k]).wait()

            @pl.when(a > 0)
            def _():
                pq_copy(a - 1).wait()

            regroup_q(side_refs[k], pst)
            pq_copy(a).start()

        @pl.when(a >= 2 * heads)
        def _():
            o_copy(w_o.at[1], k, side_refs[k]).wait()

            @pl.when(a > 2 * heads)
            def _():
                po_copy(a - 2 * heads - 1).wait()

            regroup_o(side_refs[k], pm)
            po_copy(a - 2 * heads).start()

    def start_second(k):
        if k == 0:
            second(0)[0].start()
            return

        @pl.when(core == 0)
        def _():
            own_ud(1)[k - 1].start()

        @pl.when(core == 1)
        def _():
            staged_ud(0)[k - 1].start()

        for c in second(k)[1:]:
            c.start()

    def second(k):
        if k == 0:
            return [pltpu.make_async_copy(pq, wq_v, s_rl.at[0])]
        outs = [pltpu.make_async_copy(po.at[pl.ds(h * ow, ow)], wod_v.at[pl.ds(h * hw, ow)], s_rl.at[1 + h]) for h in range(2)]
        return [staged_ud(h)[k - 1] for h in range(2)] + (outs if k == 2 else [])

    def wait_ud(i, k):
        @pl.when(i == 0)
        def _():
            own_ud(0)[k].wait()

        @pl.when(i == 2)
        def _():
            push(2 + k).wait_recv()

        @pl.when(i == items + 1)
        def _():
            for c in second(1 + k):
                c.wait()

    def weights_here(first, last, mate_pieces):
        @pl.when(core == 0)
        def _():
            for k in mate_pieces:
                push2(k).wait_recv()

        @pl.when(core == 1)
        def _():
            for j in range(first, last):
                group_bytes(0, s_gp.at[j]).wait_recv()

    def x_load(i):
        t = i - 1

        @pl.when(i == 0)
        def _():
            pltpu.make_async_copy(act.at[pl.ds(pl.multiple_of(mate_base, ROWS), ROWS)], x_v, s_x).start()

        @pl.when((i >= 1) & (t < items))
        def _():
            pltpu.make_async_copy(act.at[rows1(t, 0, ROWS)], x_v, s_x).start()

        @pl.when(t >= items)
        def _():
            q = lax.div(t - items, blocks)

            @pl.when((lax.rem(t, blocks) == 0) & (lax.rem(q, CORES) != core))
            def _():
                seq = out.at[pl.ds(0, blocks * ROWS)]
                remote(seq, seq, s_y1.at[0], s_y1.at[1 + lax.div(q, CORES)], mate).wait_recv()

            pltpu.make_async_copy(out.at[rows2(t, pair, 0, ROWS)], x_v, s_x).start()

    def x_wait():
        pltpu.make_async_copy(act.at[pl.ds(0, ROWS)], x_v, s_x).wait()

    def sl(t):
        return lax.rem(t, 2)

    def s3(t):
        return lax.rem(t, 3)

    def nth(t):
        return lax.div(t, 2 * blocks) * blocks + lax.rem(t, blocks)

    def prow(t, off, size):
        return (s3(t), at(0, off, size))

    def a1(t):
        off = jnp.where(owner(t), 1 - odd, odd) * half
        return remote(p_v.at[prow(t, off, half)], ar.at[s3(t)], s_as.at[s3(t)], s_ar.at[s3(t)], inn_d)

    def b1(t):
        return remote(ar.at[s3(t)], br, s_bs.at[0], s_br.at[0], outn_d)

    def c1(t):
        rows = rows1(t, odd * half, half)
        return [
            remote(ysh, out.at[rows], s_cs.at[0, 0], s_cr.at[0, lax.rem(t, 4)], inn_d),
            remote(ysh, out.at[rows], s_cs.at[0, 1], s_y1.at[1 + lax.div(t, 2 * blocks)], mate),
        ]

    def l1(t):
        return pltpu.make_async_copy(ysh, out.at[rows1(t, odd * half, half)], s_yl.at[0])

    def d1(t):
        rows = rows1(t, (1 - odd) * half, half)
        return remote(out.at[rows], out.at[rows], s_ds.at[0, sl(t)], s_y1.at[1 + lax.div(t, 2 * blocks)], mate)

    def r1(t):
        return pltpu.make_async_copy(act.at[rows1(t, odd * half, half)], ysh, s_xr.at[0])

    def a2(t):
        return remote(p_v.at[prow(t, (1 - core) * half, half)], pm.at[at(0, sl(t) * half, half)], s_as.at[3], s_ar2.at[sl(t)], mate)

    def b2(t):
        return remote(pm.at[at(0, sl(t) * half + (1 - odd) * quart, quart)], br2.at[sl(t)], s_bs.at[1], s_br2.at[sl(t)], inn_d)

    def c2(t):
        rows = rows2(t, pair, core * half + odd * quart, quart)
        return [
            remote(ysh2, out.at[rows], s_cs.at[1, 0], s_cr.at[1, lax.rem(t, 4)], inn_d),
            remote(ysh2, out.at[rows], s_cs.at[1, 1], s_co.at[lax.rem(t, 4)], outn_d),
        ]

    def l2(t):
        return pltpu.make_async_copy(ysh2, out.at[rows2(t, pair, core * half + odd * quart, quart)], s_yl.at[1])

    def d2(t):
        rows = rows2(t, pair, core * half + (1 - odd) * quart, quart)
        return remote(out.at[rows], out.at[rows], s_ds.at[1, sl(t)], s_do.at[lax.rem(t, 4)], outn_d)

    def r2(t):
        return pltpu.make_async_copy(out.at[rows2(t, pair, core * half + odd * quart, quart)], ysh2, s_xr.at[1])

    def f2(t, group):
        copies = []
        for p in (pair, 1 - pair):
            rows = rows2(t, p, core * half, half)
            copies.append(remote(out.at[rows], out.at[rows], s_f.at[0, group], s_f.at[1, group], mate))
        return copies

    def f32(x):
        return x.astype(F32)

    def by_rows(n, f):
        @pl.loop(0, n // 16)
        def _(i):
            f(lambda base=0: pl.ds(pl.multiple_of(base + i * 16, 16), 16))

    def slot_free(t):
        @pl.when(t + 3 < items)
        def _():
            pl.semaphore_signal(s_ca, inc=1, device_id=inn_d, device_id_type=MESH)

    def phase_a(t):
        @pl.when(t < items)
        def _():
            @pl.when(t >= 3)
            def _():
                pl.semaphore_wait(s_ca, 1)

            a1(t).start()

            @pl.when((t == 0) & owner(t))
            def _():
                r1(t).start()

        @pl.when(t >= items)
        def _():
            @pl.when(t == items)
            def _():
                pl.semaphore_wait(s_rdy, 1)

            a2(t).start()

            @pl.when(t == items)
            def _():
                r2(t).start()

    def phase_b1(t):
        @pl.when(jnp.logical_not(owner(t)))
        def _():
            n = nth(t)

            @pl.when(n > 0)
            def _():
                pl.semaphore_wait(s_cb, 1)

            a1(t).wait_recv()
            k = s3(t)

            def add(rows):
                ar[k, rows(), :] = (f32(p_v[k, rows((1 - odd) * half), :]) + f32(ar[k, rows(), :])).astype(BF16)

            by_rows(half, add)
            b1(t).start()

    def phase_c1(t):
        a1(t).wait_send()

        @pl.when(jnp.logical_not(owner(t)))
        def _():
            b1(t).wait_send()
            slot_free(t)

        @pl.when(owner(t))
        def _():
            a1(t).wait_recv()
            b1(t).wait_recv()
            r1(t).wait()
            k = s3(t)

            def add(rows):
                summed = f32(p_v[k, rows(odd * half), :]) + f32(ar[k, rows(), :]) + f32(br[rows(), :])
                ysh[rows(), :] = (f32(ysh[rows(), :]) + f32(summed.astype(BF16))).astype(BF16)

            by_rows(half, add)
            slot_free(t)

            @pl.when(nth(t) + 1 < items // 2)
            def _():
                pl.semaphore_signal(s_cb, inc=1, device_id=outn_d, device_id_type=MESH)

            for c in c1(t):
                c.start()
            l1(t).start()

    def phase_d1(t):
        @pl.when(owner(t))
        def _():
            c1(t)[0].wait_recv()
            l1(t).wait()
            for c in c1(t):
                c.wait_send()
            d1(t).start()

        @pl.when((t + 1 < items) & owner(t + 1))
        def _():
            r1(t + 1).start()

    def phase_e1(t):
        @pl.when(owner(t))
        def _():
            d1(t).wait_send()

    def phase_b2(t):
        a2(t).wait_recv()
        k, m = s3(t), sl(t) * half

        def add(rows):
            pm[rows(m + (1 - odd) * quart), :] = (f32(p_v[k, rows(core * half + (1 - odd) * quart), :]) + f32(pm[rows(m + (1 - odd) * quart), :])).astype(BF16)

        by_rows(quart, add)
        b2(t).start()

    def phase_c2(t):
        a2(t).wait_send()
        b2(t).wait_recv()
        r2(t).wait()
        k, k2, m = s3(t), sl(t), sl(t) * half

        def add(rows):
            summed = f32(p_v[k, rows(core * half + odd * quart), :]) + f32(pm[rows(m + odd * quart), :]) + f32(br2[k2, rows(), :])
            ysh2[rows(), :] = (f32(ysh2[rows(), :]) + f32(summed.astype(BF16))).astype(BF16)

        by_rows(quart, add)
        for c in c2(t):
            c.start()
        l2(t).start()
        b2(t).wait_send()

    def phase_d2(t):
        c2(t)[0].wait_recv()
        l2(t).wait()
        for c in c2(t):
            c.wait_send()
        d2(t).start()

        @pl.when(t + 1 < total)
        def _():
            r2(t + 1).start()

    def phase_e2(t):
        d2(t).wait_send()
        c2(t)[1].wait_recv()
        d2(t).wait_recv()

        @pl.when(t < total - late)
        def _():
            for c in f2(t, 0):
                c.start()

        @pl.when(t >= total - late)
        def _():
            for c in f2(t, 1):
                c.start()

    def lagged(phase, t, layer):
        lo, hi = layer * items, (layer + 1) * items

        @pl.when((t >= lo) & (t < hi))
        def _():
            phase(t)

    lane = lax.broadcasted_iota(jnp.int32, (ROWS, LANES), 1)

    def layer_norm(l):
        step = LN_ROWS

        @pl.loop(0, ROWS // step)
        def _(i):
            r = pl.ds(pl.multiple_of(i * step, step), step)
            xf = x_v[r, :].astype(F32)
            mean = jnp.mean(xf, axis=-1, keepdims=True)
            centered = xf - mean
            var = jnp.mean(centered * centered, axis=-1, keepdims=True)
            n_v[r, :] = (centered * lax.rsqrt(var + LN_EPS) * gain[pl.ds(l, 1), :] + bias[pl.ds(l, 1), :]).astype(BF16)

    def tab_copy(blk):
        return pltpu.make_async_copy(tab.at[pl.ds(pl.multiple_of(blk * ROWS, ROWS), ROWS)], tab_v, s_tab)

    def qkv(blk, g):
        rows = pl.ds(pl.multiple_of(blk * ROWS, ROWS), ROWS)
        y = jnp.dot(n_v[...], wq_v[g], preferred_element_type=F32)
        t0, t1 = y[:, :LANES], y[:, LANES:]
        cs, sn = tab_v[:, :LANES], tab_v[:, LANES:]
        for k, v in enumerate((t0 * cs - t1 * sn, t1 * cs + t0 * sn)):
            cols = pl.ds(k * LANES, LANES)
            q_v[g, :, cols] = jnp.where(lane < half_dim, v, 0.0).astype(BF16)
            kv_v[g, rows, cols] = pltpu.roll(v, LANES - half_dim, 1).astype(BF16)

    def qkv_half():
        @pl.loop(0, heads, step=2)
        def _(g):
            for j in range(2):
                qkv(jnp.int32(0), g + j)

    def attend(g, n):
        scores = lax.dot_general(q_v[g], kv_v[g, :n, :], (((1,), (1,)), ((), ())), preferred_element_type=F32)
        ri = lax.broadcasted_iota(jnp.int32, (ROWS, ROWS), 0)
        ci = lax.broadcasted_iota(jnp.int32, (ROWS, ROWS), 1)
        diag = jnp.where(ri >= ci, scores[:, n - ROWS:], -1e30)
        scores = jnp.concatenate([scores[:, :n - ROWS], diag], axis=1) if n > ROWS else diag
        e = jnp.exp2((scores - jnp.max(scores, axis=1, keepdims=True)) * np.float32(head_dim ** -0.5 * np.log2(np.e)))
        probs = (e * (1.0 / jnp.sum(e, axis=1, keepdims=True))).astype(BF16)
        return jnp.dot(probs, kv_v[g, :n, :], preferred_element_type=F32)

    def four_heads(h, n):
        base = h * hw
        ctx = [attend(h * heads + j, n) for j in range(heads)]
        for k in range(2):
            first, second, third, fourth = (c[:, k * LANES:(k + 1) * LANES] for c in ctx)
            v = jnp.where(lane < half_dim, pltpu.roll(first, LANES - half_dim, 1), second)
            w = jnp.where(lane < 3 * half_dim, pltpu.roll(third, half_dim, 1), 0.0)
            cu_v[:, pl.ds(pl.multiple_of(base + k * LANES, LANES), LANES)] = jnp.where(lane < 2 * half_dim, v, w).astype(BF16)
            v = jnp.where(lane < half_dim, pltpu.roll(fourth, LANES - half_dim, 1), 0.0)
            cu_v[:, pl.ds(pl.multiple_of(base + (2 + k) * LANES, LANES), LANES)] = v.astype(BF16)

    def attention(blk):
        for i in range(blocks):
            @pl.when(blk == i)
            def _():
                if i < UNROLLED:
                    for h in range(2):
                        four_heads(h, (i + 1) * ROWS)
                else:
                    pl.loop(0, 2)(lambda h: four_heads(h, (i + 1) * ROWS))

    tile = 2 * LANES

    def cols(n):
        return pl.ds(pl.multiple_of(n * tile, tile), tile)

    def up(h, n):
        y = jnp.dot(n_v[...], wu_v[:, cols(h * (ff // tile) + n)], preferred_element_type=F32)
        u = 0.5 * y * (1.0 + lax.erf(y * np.float32(0.5 ** 0.5)))
        cu_v[:, cols((h * hw + ow) // tile + n)] = u.astype(BF16)

    def down(depth, slot, n):
        y = jnp.dot(cu_v[:, :depth], wod_v[:depth, cols(n)], preferred_element_type=F32)
        p_v[slot, :, cols(n)] = y.astype(BF16)

    def pm_copy():
        return remote(p_v.at[0], pm, s_pm.at[0], s_pm.at[1], mate)

    def f_wait(count, group):
        rows = out.at[pl.ds(0, count * ROWS)]
        both = remote(rows, rows, s_f.at[0, group], s_f.at[1, group], mate)
        both.wait_send()
        both.wait_recv()

    in_u, in_od = d_model, 2 * hw

    def final_load(k):
        if k == 0:
            return pltpu.make_async_copy(out.at[pl.ds(0, in_u)], wu_v, s_fin.at[0])
        return pltpu.make_async_copy(out.at[pl.ds(in_u, in_od)], wod_v, s_fin.at[1])

    def send_group(i, k):
        for j in range(2, len(groups)):
            @pl.when((i == j) & (core == twin))
            def _():
                group_send(j, k).start()

    barrier = pltpu.get_barrier_semaphore()
    for d in (inn_d, outn_d, mate, dev(outn, CORES - 1 - core), peer):
        pl.semaphore_signal(barrier, inc=1, device_id=d, device_id_type=MESH)
    x_load(jnp.int32(0))
    tab_copy(jnp.int32(0)).start()
    for g in range(len(slots)):
        q_copy(g).start()
    pl.semaphore_wait(barrier, 5)

    @pl.when(core == twin)
    def _():
        for j in range(2):
            for k in range(4):
                group_send(j, k).start()

    @pl.loop(0, total + 4)
    def _(i):
        t = i - 1
        tc = jnp.maximum(t, 0)
        compute = i <= total
        small = i < 2
        whole = (i >= 2) & compute
        blk = lax.rem(tc, blocks)
        job = (t - side_at) * 2
        has_jobs = (t >= side_at) & (t < side_at + n_side // 2)

        def on(cond):
            return pl.when(cond)

        @on(i == 0)
        def _():
            load_q()
            clear_tail(slots[1])
            for k in range(2):
                o_copy(w_o.at[0], k, slots[k]).start()
            for c in own_ud(0):
                c.start()

        @on(compute)
        def _():
            x_wait()
            layer_norm(lax.div(tc, items))

            @on(i < total)
            def _():
                x_load(i + 1)

        @on(i == 0)
        def _():
            push(0).start()

        send_group(i, 0)
        for j in range(len(groups)):
            @on((t == j + 1) & (core == 1))
            def _():
                group_bytes(1, s_gx.at[j]).wait_recv()
                for c in group_pass(j):
                    c.start()

        @on(t == items)
        def _():
            for c in second(0):
                c.wait()

        @on(i == 1)
        def _():
            push_kv().wait_send()

        @on(i == 2)
        def _():
            push(0).wait_recv()
            push_kv().wait_recv()

        @on(compute & (i != 1))
        def _():
            tab_copy(blk).wait()

        @on(small)
        def _():
            qkv_half()

        @on(whole)
        def _():
            for g in range(2 * heads):
                qkv(blk, g)

        @on((i >= 1) & (i < total))
        def _():
            tab_copy(lax.rem(i, blocks)).start()

        lagged(phase_b2, t - 1, 1)

        @on((t > side_at) & (t <= side_at + n_side // 2))
        def _():
            side_job(job - 1, 1)

        @on(t == items - 1)
        def _():
            pq_copy(0).wait()
            po_copy(0).wait()
            pl.semaphore_signal(s_rdy, inc=1, device_id=mate, device_id_type=MESH)
            start_second(0)

        send_group(i, 1)

        @on(small)
        def _():
            four_heads(0, ROWS)

        @on(i == 0)
        def _():
            push_kv().start()

        @on(whole)
        def _():
            attention(blk)

        send_group(i, 2)

        @on(compute)
        def _():
            wait_ud(i, 0)

            @on(small)
            def _():
                pl.loop(0, ff // tile)(lambda n: up(0, n))

            @on(whole)
            def _():
                for h in range(2):
                    for n in range(ff // tile):
                        up(h, n)

        @on(has_jobs)
        def _():
            side_copy(job, 0)

        @on(t == items - 1)
        def _():
            weights_here(5, 10, (2,))
            start_second(1)

        @on(t == total - 1)
        def _():
            f_wait(items - late, 0)
            final_load(0).start()

        lagged(phase_e1, t - 5, 0)
        lagged(phase_e2, t - 3, 1)
        lagged(phase_d1, t - 4, 0)
        lagged(phase_d2, t - 2, 1)
        lagged(phase_c1, t - 3, 0)
        lagged(phase_b1, t - 2, 0)
        send_group(i, 3)

        @on(small)
        def _():
            @on(i == 0)
            def _():
                load_o()

            @on(i == 1)
            def _():
                pm_copy().wait_send()

            wait_ud(i, 1)

            @pl.loop(0, d_model // tile, step=2)
            def _(n):
                for k in range(2):
                    down(hw, 0, n + k)

            @on(i == 0)
            def _():
                pm_copy().start()
                for k in range(1, 4):
                    push(k).start()

            @on(i == 1)
            def _():
                pm_copy().wait_recv()

                def add(rows):
                    p_v[0, rows(), :] = (f32(p_v[0, rows(), :]) + f32(pm[rows(), :])).astype(BF16)

                by_rows(ROWS, add)

        @on(i == 2)
        def _():
            push(1).wait_recv()

        @on(whole)
        def _():
            wait_ud(i, 1)
            for n in range(d_model // tile):
                down(2 * hw, s3(t), n)

        lagged(phase_c2, t - 1, 1)

        @on((i >= 1) & compute)
        def _():
            phase_a(t)

        @on(has_jobs)
        def _():
            side_copy(job + 1, 1)
            side_job(job, 0)

        @on(t == items - 1)
        def _():
            weights_here(10, len(groups), (3,))
            start_second(2)

        @on(t == total - 1)
        def _():
            final_load(1).start()

        @on(t == 2)
        def _():
            for k in range(4):
                push(k).wait_send()

            @on(core == 1)
            def _():
                for k in range(4):
                    push2(k).start()

        @on(t == side_at - 1)
        def _():
            weights_here(0, 5, (0, 1))


    @pl.when(core == 1)
    def _():
        for i in range(4):
            push2(i).wait_send()
        group_bytes(1, s_gx.at[0], len(groups)).wait_send()

    @pl.when(core == twin)
    def _():
        group_bytes(0, s_gx.at[0], len(groups)).wait_send()

    f_wait(late, 1)
    for k in range(2):
        final_load(k).wait()


def collect(y, va, vb, out, buf, sem):
    na, nb = va.shape[0], vb.shape[0]
    spans = [pl.ds(na + nb + n * ROWS, ROWS) for n in range(buf.shape[0])]
    ins = [pltpu.make_async_copy(y.at[r], buf.at[n], sem.at[2 + n]) for n, r in enumerate(spans)]
    outs = [pltpu.make_async_copy(buf.at[n], out.at[r], sem.at[2 + n]) for n, r in enumerate(spans)]
    direct = [
        pltpu.make_async_copy(va, out.at[pl.ds(0, na)], sem.at[0]),
        pltpu.make_async_copy(vb, out.at[pl.ds(na, nb)], sem.at[1]),
    ]
    for c in ins + direct:
        c.start()
    for c, d in zip(ins, outs):
        c.wait()
        d.start()
    for c in direct + outs:
        c.wait()


def solution(mesh):
    n_tp = mesh.shape["tp"]
    n_chip = n_tp // CORES

    def shard_body(act_in, ln_gain, ln_bias, w_qkv, w_out, w_up, w_down):
        batch, seq_len, d_model = act_in.shape
        layers, _, heads, group_cols = w_qkv.shape
        head_dim = w_out.shape[1] // heads
        ff = w_up.shape[2]
        assert group_cols == 3 * head_dim and heads == 4 and head_dim == 2 * SLOT
        items = batch * seq_len // (CORES * ROWS)
        blocks = seq_len // ROWS
        late = 4
        cfg = (n_chip, layers, heads, head_dim, d_model, ff, items, blocks, late)
        ow = 4 * LANES
        quart = ROWS // 4
        n_groups = (heads * group_cols + heads * head_dim + d_model // 2 + ff) // ROWS
        w_q = jnp.transpose(w_qkv, (0, 2, 3, 1)).reshape(layers, heads * group_cols, d_model)
        vm = pl.BlockSpec(memory_space=pltpu.VMEM)
        hb = pl.BlockSpec(memory_space=pl.ANY)
        dma = pltpu.SemaphoreType.DMA
        two, three, four, square, many = (dma(n) for n in ((2,), (3,), (4,), (2, 2), (n_groups,)))
        plain = pltpu.SemaphoreType.REGULAR
        out_vmem = (d_model * 2 * ff + (2 * ow + 2 * ff) * d_model) * 2
        res = pl.pallas_call(
            functools.partial(body, cfg),
            name="layers",
            out_shape=[
                jax.ShapeDtypeStruct((batch * seq_len, d_model), BF16),
                pltpu.VMEM((d_model, 2 * ff), BF16),
                pltpu.VMEM((2 * ow + 2 * ff, d_model), BF16),
                jax.ShapeDtypeStruct((2, heads * group_cols, d_model), BF16),
                jax.ShapeDtypeStruct((2, heads * head_dim, d_model), BF16),
                jax.ShapeDtypeStruct((2, d_model, ff), BF16),
                jax.ShapeDtypeStruct((2, ff, d_model), BF16),
                jax.ShapeDtypeStruct((2 * heads, d_model, 2 * LANES), BF16),
                jax.ShapeDtypeStruct((2 * ow, d_model), BF16),
            ],
            in_specs=[hb] * 5 + [vm] * 2 + [hb, vm],
            out_specs=[hb, vm, vm] + [hb] * 6,
            scratch_shapes=[
                pltpu.VMEM((ROWS, 2 * LANES), F32),
                pltpu.VMEM((d_model, 2 * LANES), BF16),
                pltpu.VMEM((ROWS, d_model), BF16),
                pltpu.VMEM((ROWS, d_model), BF16),
                pltpu.VMEM((ROWS, d_model), BF16),
                pltpu.VMEM((2 * heads, ROWS, 2 * LANES), BF16),
                pltpu.VMEM((2 * heads, seq_len, 2 * LANES), BF16),
                pltpu.VMEM((ROWS, 2 * ow + 2 * ff), BF16),
                pltpu.VMEM((3, ROWS, d_model), BF16),
                pltpu.VMEM((2 * heads, d_model, 2 * LANES), BF16),
                pltpu.VMEM((3, 2 * quart, d_model), BF16),
                pltpu.VMEM((2 * quart, d_model), BF16),
                pltpu.VMEM((2 * quart, d_model), BF16),
                pltpu.VMEM((2, quart, d_model), BF16),
                pltpu.VMEM((quart, d_model), BF16),
                four, three, two, two, two, two, square, dma((layers, 4)), four, square, four, three, two,
                dma, two, square, square, four, four, four, four,
                two, many, many, three, two, two, three, two,
                dma, two, plain, plain, plain,
            ],
            compiler_params=pltpu.CompilerParams(collective_id=0, has_side_effects=True, vmem_limit_bytes=VMEM_LIMIT - out_vmem),
        )(act_in.reshape(batch * seq_len, d_model), w_q, w_out, w_up, w_down, ln_gain, ln_bias, jnp.asarray(rope_tables(seq_len, head_dim)), jnp.asarray(regroup(head_dim), BF16))
        rest = batch * seq_len // ROWS - (d_model + 2 * ow + 2 * ff) // ROWS
        y = pl.pallas_call(
            collect,
            name="collect",
            out_shape=jax.ShapeDtypeStruct((batch * seq_len, d_model), BF16),
            in_specs=[hb, vm, vm],
            out_specs=hb,
            scratch_shapes=[pltpu.VMEM((rest, ROWS, d_model), BF16), dma((2 + rest,))],
            compiler_params=pltpu.CompilerParams(vmem_limit_bytes=16 << 20),
        )(*res[:3])
        return y.reshape(batch, seq_len, d_model)

    wide = P(None, None, "tp")
    tall = P(None, "tp")
    return jax.shard_map(shard_body, mesh=mesh, in_specs=(P("dp"), P(), P(), wide, tall, wide, tall), out_specs=P("dp"), check_vma=False)
```

```python
import functools

import jax
import jax.numpy as jnp
import numpy as np
from jax import lax
from jax.experimental import pallas as pl
from jax.experimental.pallas import tpu as pltpu
from jax.sharding import PartitionSpec as P

LN_EPS = 1e-5
ROPE_BASE = 10000.0
F32 = jnp.float32
BF16 = jnp.bfloat16
MESH = pl.DeviceIdType.MESH
VMEM_LIMIT = 67043328

CORES = 2
ROWS = 256
LANES = 128
SLOT = 40
LN_ROWS = 128
UNROLLED = 3


def rope_tables(seq_len, head_dim):
    half_dim = head_dim // 2
    inv_freq = (ROPE_BASE ** (-2.0 * np.arange(half_dim, dtype=np.float32) / head_dim)).astype(np.float32)
    angles = np.arange(seq_len, dtype=np.float32)[:, None] * inv_freq[None, :]
    cos_tab = np.ones((seq_len, LANES), np.float32)
    sin_tab = np.zeros((seq_len, LANES), np.float32)
    for k in range(2):
        cos_tab[:, k * half_dim:(k + 1) * half_dim] = np.cos(angles)
        sin_tab[:, k * half_dim:(k + 1) * half_dim] = np.sin(angles)
    return np.concatenate([cos_tab, sin_tab], axis=1)


def regroup(head_dim):
    half_dim = head_dim // 2
    sel = np.zeros((3 * head_dim, 2 * LANES), np.float32)
    for part in range(3):
        for half in range(2):
            for i in range(half_dim):
                sel[(part * 2 + half) * half_dim + i, half * LANES + part * half_dim + i] = 1.0
    return sel


def body(cfg, act, w_q, w_o, w_u, w_d, gain, bias, tab, sel_v,
         out, wu_v, wod_v, st_q, st_o, st_u, st_d, pq, po,
         tab_v, pst, pm, x_v, n_v, q_v, kv_v, cu_v, p_v, wq_v,
         ar, br, ysh, br2, ysh2,
         s_as, s_ar, s_ar2, s_bs, s_br, s_br2, s_cs, s_cr, s_cr2, s_co, s_ds, s_do, s_y1, s_yl, s_x, s_xr, s_f, s_wl, s_ws, s_wr, s_m2s, s_m2r,
         s_gs, s_gx, s_gp, s_stg, s_pm, s_pq, s_rl, s_fin, s_tab, s_kv, s_ca, s_cb, s_rdy):
    n_chip, layers, heads, head_dim, d_model, ff, items, blocks, late = cfg
    side_at = 9
    group_cols = 3 * head_dim
    seq_blocks = blocks
    group_cols = 3 * head_dim
    half_dim = head_dim // 2
    total = layers * items
    tp = lax.axis_index("tp")
    dp = lax.axis_index("dp")
    chip = lax.div(tp, CORES)
    core = lax.rem(tp, CORES)
    twin = lax.rem(dp, 2)
    odd = lax.rem(chip, 2)
    pair = lax.div(chip, 2)
    inn = chip + 1 - 2 * odd
    outn = lax.rem(chip + n_chip - 1 + 2 * odd, n_chip)

    def dev(c, k):
        return {"tp": c * CORES + k}

    inn_d, outn_d, mate = dev(inn, core), dev(outn, core), dev(chip, CORES - 1 - core)
    peer = {"dp": dp + 1 - 2 * twin, "tp": tp}
    own_base = core * (items * ROWS)
    mate_base = (CORES - 1 - core) * (items * ROWS)
    half = ROWS // 2
    quart = ROWS // 4
    ow = 4 * LANES
    hw = ow + ff

    def remote(src, dst, ssem, rsem, dev):
        return pltpu.make_async_remote_copy(src_ref=src, dst_ref=dst, send_sem=ssem, recv_sem=rsem, device_id=dev, device_id_type=MESH)

    def at(base, off, size):
        return pl.ds(pl.multiple_of(base + off, min(size, quart)), size)

    def rows1(t, off, size):
        return at(own_base + lax.rem(t, items) * ROWS, off, size)

    def rows2(t, p, off, size):
        u = t - items
        q = lax.div(u, blocks)
        cc = lax.rem(q, CORES)
        seq = p + cc - 2 * p * cc + 2 * lax.div(q, CORES)
        return at(cc * (items * ROWS) + (seq * blocks + lax.rem(u, blocks)) * ROWS, off, size)

    def owner(t):
        return lax.rem(lax.div(t, blocks) + core, 2) == pair

    def ud_dst(h):
        return [wu_v.at[:, pl.ds(h * ff, ff)], wod_v.at[pl.ds(h * hw + ow, ff)]]

    def own_ud(l):
        return [pltpu.make_async_copy(s.at[l], d, s_wl.at[0, i]) for i, (s, d) in enumerate(zip((w_u, w_d), ud_dst(0)))]

    def staged_ud(h):
        return [pltpu.make_async_copy(s.at[h], d, s_wl.at[h, i]) for i, (s, d) in enumerate(zip((st_u, st_d), ud_dst(h)))]

    def push(i):
        src = (wq_v.at[pl.ds(0, heads)], wod_v.at[pl.ds(0, ow)], w_u.at[0], w_d.at[0])[i]
        dst = (wq_v.at[pl.ds(heads, heads)], wod_v.at[pl.ds(hw, ow)], *ud_dst(1))[i]
        return remote(src, dst, s_ws.at[i], s_wr.at[i], mate)

    def push_kv():
        rows = pl.ds(0, ROWS)
        return remote(kv_v.at[pl.ds(0, heads), rows], kv_v.at[pl.ds(heads, heads), rows], s_kv.at[0], s_kv.at[1], mate)

    args2 = (w_q.at[1], w_o.at[1], w_u.at[1], w_d.at[1])
    staged = (st_q, st_o, st_u, st_d)

    def push2(i):
        return remote(args2[i], staged[i].at[1], s_m2s.at[i], s_m2r.at[i], mate)

    pieces = []
    for k, (n_rows, step) in enumerate(((heads * group_cols, quart), (heads * head_dim, quart), (d_model, 2 * quart), (ff, quart))):
        pieces += [(k, r, step) for r in range(0, n_rows, step)]
    groups = [pieces[j:j + 4] for j in range(0, len(pieces), 4)]

    def group_send(j, k):
        arr, r, n = groups[j][k]
        rows = pl.ds(r, n)
        return remote(args2[arr].at[rows], staged[arr].at[twin, rows], s_gs.at[0], s_gx.at[j], dev(outn, 1))

    def group_pass(j):
        copies = []
        for arr in range(4):
            mine = [p for p in groups[j] if p[0] == arr]
            if mine:
                rows = pl.ds(mine[0][1], sum(p[2] for p in mine))
                copies.append(remote(staged[arr].at[twin, rows], staged[arr].at[twin, rows], s_gs.at[1], s_gp.at[j], peer))
        return copies

    def group_bytes(j, sem, n=1):
        rows = out.at[pl.ds(0, n * ROWS)]
        return remote(rows, rows, s_gs.at[j], sem, peer)

    def regroup_q(src, dst, unroll=False):
        def one(c):
            part = pl.ds(c, 512) if unroll else pl.ds(pl.multiple_of(c, 512), 512)
            y = lax.dot_general(src[:, part], sel_v[...], (((0,), (0,)), ((), ())), preferred_element_type=F32)
            dst[part, :] = y.astype(BF16)

        if unroll:
            for c in range(0, d_model, 512):
                one(c)
        else:
            pl.loop(0, d_model, step=512)(one)

    def regroup_o(src, dst, unroll=False):
        def one(c):
            part = pl.ds(c, 512) if unroll else pl.ds(pl.multiple_of(c, 512), 512)
            y = lax.dot_general(sel_v[...], src[:, part], (((0,), (0,)), ((), ())), preferred_element_type=F32)
            dst[:, part] = y.astype(BF16)

        if unroll:
            for c in range(0, d_model, 512):
                one(c)
        else:
            pl.loop(0, d_model, step=512)(one)

    def slot(k):
        return p_v.at[k, pl.ds(0, group_cols)]

    n_slots = 3

    def q_copy(g):
        rows = pl.ds(pl.multiple_of(g * group_cols, group_cols), group_cols)
        k = lax.rem(g, n_slots)
        return pltpu.make_async_copy(w_q.at[0, rows], slot(k), s_stg.at[k])

    def load_q():
        @pl.loop(0, heads)
        def _(g):
            q_copy(g).wait()
            regroup_q(slot(lax.rem(g, n_slots)), wq_v.at[g], True)

            @pl.when(g + n_slots < heads)
            def _():
                q_copy(g + n_slots).start()

    def o_copy(src, k, dst):
        rows = (pl.ds(0, group_cols), pl.ds(group_cols, head_dim))[k]
        return pltpu.make_async_copy(src.at[rows], dst.at[pl.ds(0, (group_cols, head_dim)[k])], s_stg.at[k])

    def clear_tail(ref):
        ref[pl.ds(head_dim, group_cols - head_dim), :] = jnp.zeros((group_cols - head_dim, d_model), BF16)

    def load_o():
        for k in range(2):
            o_copy(w_o.at[0], k, slot(k)).wait()

        @pl.loop(0, 2)
        def _(k):
            regroup_o(slot(k), wod_v.at[pl.ds(pl.multiple_of(k * 2 * LANES, 2 * LANES), 2 * LANES)], True)

    n_side = 2 * heads + 4
    side_refs = (n_v.at[pl.ds(0, group_cols)], cu_v.at[pl.ds(0, group_cols), pl.ds(0, d_model)])

    def side_copy(a, k):
        for h in range(2):
            for arg in range(2 - h):
                from_arg = (core == 0) if arg else ((core == 1) if h == 0 else (core >= 0))

                @pl.when((a >= h * heads) & (a < (h + 1) * heads) & from_arg)
                def _():
                    rows = pl.ds(pl.multiple_of((a - h * heads) * group_cols, group_cols), group_cols)
                    src = w_q.at[1, rows] if arg else st_q.at[h, rows]
                    pltpu.make_async_copy(src, side_refs[k], s_stg.at[k]).start()

                @pl.when((a == 2 * heads + 2 * h + k) & from_arg)
                def _():
                    if k:
                        clear_tail(side_refs[k])
                    o_copy(w_o.at[1] if arg else st_o.at[h], k, side_refs[k]).start()

    def pq_copy(g):
        return pltpu.make_async_copy(pst, pq.at[g], s_pq.at[0])

    def po_copy(b):
        return pltpu.make_async_copy(pm, po.at[pl.ds(pl.multiple_of(b * 2 * LANES, 2 * LANES), 2 * LANES)], s_pq.at[1])

    def side_job(a, k):
        @pl.when(a < 2 * heads)
        def _():
            pltpu.make_async_copy(w_q.at[1, pl.ds(0, group_cols)], side_refs[k], s_stg.at[k]).wait()

            @pl.when(a > 0)
            def _():
                pq_copy(a - 1).wait()

            regroup_q(side_refs[k], pst)
            pq_copy(a).start()

        @pl.when(a >= 2 * heads)
        def _():
            o_copy(w_o.at[1], k, side_refs[k]).wait()

            @pl.when(a > 2 * heads)
            def _():
                po_copy(a - 2 * heads - 1).wait()

            regroup_o(side_refs[k], pm)
            po_copy(a - 2 * heads).start()

    def start_second(k):
        if k == 0:
            second(0)[0].start()
            return

        @pl.when(core == 0)
        def _():
            own_ud(1)[k - 1].start()

        @pl.when(core == 1)
        def _():
            staged_ud(0)[k - 1].start()

        for c in second(k)[1:]:
            c.start()

    def second(k):
        if k == 0:
            return [pltpu.make_async_copy(pq, wq_v, s_rl.at[0])]
        outs = [pltpu.make_async_copy(po.at[pl.ds(h * ow, ow)], wod_v.at[pl.ds(h * hw, ow)], s_rl.at[1 + h]) for h in range(2)]
        return [staged_ud(h)[k - 1] for h in range(2)] + (outs if k == 2 else [])

    def wait_ud(i, k):
        @pl.when(i == 0)
        def _():
            own_ud(0)[k].wait()

        @pl.when(i == 2)
        def _():
            push(2 + k).wait_recv()

        @pl.when(i == items + 1)
        def _():
            for c in second(1 + k):
                c.wait()

    def weights_here(first, last, mate_pieces):
        @pl.when(core == 0)
        def _():
            for k in mate_pieces:
                push2(k).wait_recv()

        @pl.when(core == 1)
        def _():
            for j in range(first, last):
                group_bytes(0, s_gp.at[j]).wait_recv()

    def x_load(i):
        t = i - 1

        @pl.when(i == 0)
        def _():
            pltpu.make_async_copy(act.at[pl.ds(pl.multiple_of(mate_base, ROWS), ROWS)], x_v, s_x).start()

        @pl.when((i >= 1) & (t < items))
        def _():
            pltpu.make_async_copy(act.at[rows1(t, 0, ROWS)], x_v, s_x).start()

        @pl.when(t >= items)
        def _():
            q = lax.div(t - items, blocks)

            @pl.when((lax.rem(t, blocks) == 0) & (lax.rem(q, CORES) != core))
            def _():
                seq = out.at[pl.ds(0, blocks * ROWS)]
                remote(seq, seq, s_y1.at[0], s_y1.at[1 + lax.div(q, CORES)], mate).wait_recv()

            pltpu.make_async_copy(out.at[rows2(t, pair, 0, ROWS)], x_v, s_x).start()

    def x_wait():
        pltpu.make_async_copy(act.at[pl.ds(0, ROWS)], x_v, s_x).wait()

    def sl(t):
        return lax.rem(t, 2)

    def s3(t):
        return lax.rem(t, 3)

    def nth(t):
        return lax.div(t, 2 * blocks) * blocks + lax.rem(t, blocks)

    def prow(t, off, size):
        return (s3(t), at(0, off, size))

    def a1(t):
        off = jnp.where(owner(t), 1 - odd, odd) * half
        return remote(p_v.at[prow(t, off, half)], ar.at[s3(t)], s_as.at[s3(t)], s_ar.at[s3(t)], inn_d)

    def b1(t):
        return remote(ar.at[s3(t)], br, s_bs.at[0], s_br.at[0], outn_d)

    def c1(t):
        rows = rows1(t, odd * half, half)
        return [
            remote(ysh, out.at[rows], s_cs.at[0, 0], s_cr.at[lax.rem(t, 4)], inn_d),
            remote(ysh, out.at[rows], s_cs.at[0, 1], s_y1.at[1 + lax.div(t, 2 * blocks)], mate),
        ]

    def l1(t):
        return pltpu.make_async_copy(ysh, out.at[rows1(t, odd * half, half)], s_yl.at[0])

    def d1(t):
        rows = rows1(t, (1 - odd) * half, half)
        return remote(out.at[rows], out.at[rows], s_ds.at[0, sl(t)], s_y1.at[1 + lax.div(t, 2 * blocks)], mate)

    def r1(t):
        return pltpu.make_async_copy(act.at[rows1(t, odd * half, half)], ysh, s_xr.at[0])

    def a2(t):
        return remote(p_v.at[prow(t, (1 - core) * half, half)], pm.at[at(0, sl(t) * half, half)], s_as.at[3], s_ar2.at[sl(t)], mate)

    piece = quart // 2

    def b2(t, p):
        m = sl(t) * half + (1 - odd) * quart
        dst = br2.at[sl(t), pl.ds(p * piece, piece)]
        return remote(pm.at[piece_rows(m, p)], dst, s_bs.at[1], s_br2.at[sl(t), p], inn_d)

    def piece_rows(base, p):
        return pl.ds(pl.multiple_of(base + p * piece, piece), piece)

    def c2(t, p):
        rows = rows2(t, pair, core * half + odd * quart + p * piece, piece)
        src = ysh2.at[pl.ds(p * piece, piece)]
        k = lax.rem(t, 4)
        return [
            remote(src, out.at[rows], s_cs.at[1, 0], s_cr2.at[k, p], inn_d),
            remote(src, out.at[rows], s_cs.at[1, 1], s_co.at[k, p], outn_d),
        ]

    def l2(t):
        return pltpu.make_async_copy(ysh2, out.at[rows2(t, pair, core * half + odd * quart, quart)], s_yl.at[1])

    def d2(t, p):
        rows = rows2(t, pair, core * half + (1 - odd) * quart + p * piece, piece)
        return remote(out.at[rows], out.at[rows], s_ds.at[1, sl(t)], s_do.at[lax.rem(t, 4), p], outn_d)

    def sent2(sem):
        return remote(ysh2, ysh2, sem, s_cr2.at[0, 0], inn_d).wait_send()

    def r2(t):
        return pltpu.make_async_copy(out.at[rows2(t, pair, core * half + odd * quart, quart)], ysh2, s_xr.at[1])

    def f2(t, group):
        copies = []
        for p in (pair, 1 - pair):
            rows = rows2(t, p, core * half, half)
            copies.append(remote(out.at[rows], out.at[rows], s_f.at[0, group], s_f.at[1, group], mate))
        return copies

    def f32(x):
        return x.astype(F32)

    def by_rows(n, f):
        @pl.loop(0, n // 16)
        def _(i):
            f(lambda base=0: pl.ds(pl.multiple_of(base + i * 16, 16), 16))

    def slot_free(t):
        @pl.when(t + 3 < items)
        def _():
            pl.semaphore_signal(s_ca, inc=1, device_id=inn_d, device_id_type=MESH)

    def phase_a(t):
        @pl.when(t < items)
        def _():
            @pl.when(t >= 3)
            def _():
                pl.semaphore_wait(s_ca, 1)

            a1(t).start()

            @pl.when((t == 0) & owner(t))
            def _():
                r1(t).start()

        @pl.when(t >= items)
        def _():
            @pl.when(t == items)
            def _():
                pl.semaphore_wait(s_rdy, 1)

            a2(t).start()

            @pl.when(t == items)
            def _():
                r2(t).start()

    def phase_b1(t):
        @pl.when(jnp.logical_not(owner(t)))
        def _():
            n = nth(t)

            @pl.when(n > 0)
            def _():
                pl.semaphore_wait(s_cb, 1)

            a1(t).wait_recv()
            k = s3(t)

            def add(rows):
                ar[k, rows(), :] = (f32(p_v[k, rows((1 - odd) * half), :]) + f32(ar[k, rows(), :])).astype(BF16)

            by_rows(half, add)
            b1(t).start()

    def phase_c1(t):
        a1(t).wait_send()

        @pl.when(jnp.logical_not(owner(t)))
        def _():
            b1(t).wait_send()
            slot_free(t)

        @pl.when(owner(t))
        def _():
            a1(t).wait_recv()
            b1(t).wait_recv()
            r1(t).wait()
            k = s3(t)

            def add(rows):
                summed = f32(p_v[k, rows(odd * half), :]) + f32(ar[k, rows(), :]) + f32(br[rows(), :])
                ysh[rows(), :] = (f32(ysh[rows(), :]) + f32(summed.astype(BF16))).astype(BF16)

            by_rows(half, add)
            slot_free(t)

            @pl.when(nth(t) + 1 < items // 2)
            def _():
                pl.semaphore_signal(s_cb, inc=1, device_id=outn_d, device_id_type=MESH)

            for c in c1(t):
                c.start()
            l1(t).start()

    def phase_d1(t):
        @pl.when(owner(t))
        def _():
            c1(t)[0].wait_recv()
            l1(t).wait()
            for c in c1(t):
                c.wait_send()
            d1(t).start()

        @pl.when((t + 1 < items) & owner(t + 1))
        def _():
            r1(t + 1).start()

    def phase_e1(t):
        @pl.when(owner(t))
        def _():
            d1(t).wait_send()

    def phase_b2(t):
        a2(t).wait_recv()
        k, m = s3(t), sl(t) * half
        for p in range(2):
            q = (1 - odd) * quart + p * piece

            def add(rows):
                pm[rows(m + q), :] = (f32(p_v[k, rows(core * half + q), :]) + f32(pm[rows(m + q), :])).astype(BF16)

            by_rows(piece, add)
            b2(t, p).start()

    def phase_c2(t):
        a2(t).wait_send()
        r2(t).wait()
        k, k2, m = s3(t), sl(t), sl(t) * half
        for p in range(2):
            q = odd * quart + p * piece
            o = p * piece

            def add(rows):
                summed = f32(p_v[k, rows(core * half + q), :]) + f32(pm[rows(m + q), :]) + f32(br2[k2, rows(o), :])
                ysh2[rows(o), :] = (f32(ysh2[rows(o), :]) + f32(summed.astype(BF16))).astype(BF16)

            b2(t, p).wait_recv()
            by_rows(piece, add)
            for c in c2(t, p):
                c.start()
        l2(t).start()
        sent2(s_bs.at[1])

    def phase_d2(t):
        for p in range(2):
            c2(t, p)[0].wait_recv()
            d2(t, p).start()
        l2(t).wait()
        for k in range(2):
            sent2(s_cs.at[1, k])

        @pl.when(t + 1 < total)
        def _():
            r2(t + 1).start()

    def phase_e2(t):
        sent2(s_ds.at[1, sl(t)])
        for p in range(2):
            c2(t, p)[1].wait_recv()
            d2(t, p).wait_recv()

        @pl.when(t < total - late)
        def _():
            for c in f2(t, 0):
                c.start()

        @pl.when(t >= total - late)
        def _():
            for c in f2(t, 1):
                c.start()

    def lagged(phase, t, layer):
        lo, hi = layer * items, (layer + 1) * items

        @pl.when((t >= lo) & (t < hi))
        def _():
            phase(t)

    lane = lax.broadcasted_iota(jnp.int32, (ROWS, LANES), 1)

    def layer_norm(l):
        step = LN_ROWS

        @pl.loop(0, ROWS // step)
        def _(i):
            r = pl.ds(pl.multiple_of(i * step, step), step)
            xf = x_v[r, :].astype(F32)
            mean = jnp.mean(xf, axis=-1, keepdims=True)
            centered = xf - mean
            var = jnp.mean(centered * centered, axis=-1, keepdims=True)
            n_v[r, :] = (centered * lax.rsqrt(var + LN_EPS) * gain[pl.ds(l, 1), :] + bias[pl.ds(l, 1), :]).astype(BF16)

    def tab_copy(blk):
        return pltpu.make_async_copy(tab.at[pl.ds(pl.multiple_of(blk * ROWS, ROWS), ROWS)], tab_v, s_tab)

    def qkv(blk, g):
        rows = pl.ds(pl.multiple_of(blk * ROWS, ROWS), ROWS)
        y = jnp.dot(n_v[...], wq_v[g], preferred_element_type=F32)
        t0, t1 = y[:, :LANES], y[:, LANES:]
        cs, sn = tab_v[:, :LANES], tab_v[:, LANES:]
        for k, v in enumerate((t0 * cs - t1 * sn, t1 * cs + t0 * sn)):
            cols = pl.ds(k * LANES, LANES)
            q_v[g, :, cols] = jnp.where(lane < half_dim, v, 0.0).astype(BF16)
            kv_v[g, rows, cols] = pltpu.roll(v, LANES - half_dim, 1).astype(BF16)

    def qkv_half():
        for g in range(heads):
            qkv(jnp.int32(0), g)

    def attend(g, n):
        scores = lax.dot_general(q_v[g], kv_v[g, :n, :], (((1,), (1,)), ((), ())), preferred_element_type=F32)
        ri = lax.broadcasted_iota(jnp.int32, (ROWS, ROWS), 0)
        ci = lax.broadcasted_iota(jnp.int32, (ROWS, ROWS), 1)
        diag = jnp.where(ri >= ci, scores[:, n - ROWS:], -1e30)
        scores = jnp.concatenate([scores[:, :n - ROWS], diag], axis=1) if n > ROWS else diag
        e = jnp.exp2((scores - jnp.max(scores, axis=1, keepdims=True)) * np.float32(head_dim ** -0.5 * np.log2(np.e)))
        probs = (e * (1.0 / jnp.sum(e, axis=1, keepdims=True))).astype(BF16)
        return jnp.dot(probs, kv_v[g, :n, :], preferred_element_type=F32)

    def four_heads(h, n):
        base = h * hw
        ctx = [attend(h * heads + j, n) for j in range(heads)]
        for k in range(2):
            first, second, third, fourth = (c[:, k * LANES:(k + 1) * LANES] for c in ctx)
            v = jnp.where(lane < half_dim, pltpu.roll(first, LANES - half_dim, 1), second)
            w = jnp.where(lane < 3 * half_dim, pltpu.roll(third, half_dim, 1), 0.0)
            cu_v[:, pl.ds(pl.multiple_of(base + k * LANES, LANES), LANES)] = jnp.where(lane < 2 * half_dim, v, w).astype(BF16)
            v = jnp.where(lane < half_dim, pltpu.roll(fourth, LANES - half_dim, 1), 0.0)
            cu_v[:, pl.ds(pl.multiple_of(base + (2 + k) * LANES, LANES), LANES)] = v.astype(BF16)

    def attention(blk):
        for i in range(blocks):
            @pl.when(blk == i)
            def _():
                if i < UNROLLED:
                    for h in range(2):
                        four_heads(h, (i + 1) * ROWS)
                else:
                    pl.loop(0, 2)(lambda h: four_heads(h, (i + 1) * ROWS))

    tile = 2 * LANES

    def cols(n):
        return pl.ds(pl.multiple_of(n * tile, tile), tile)

    def up(h, n):
        y = jnp.dot(n_v[...], wu_v[:, cols(h * (ff // tile) + n)], preferred_element_type=F32)
        u = 0.5 * y * (1.0 + lax.erf(y * np.float32(0.5 ** 0.5)))
        cu_v[:, cols((h * hw + ow) // tile + n)] = u.astype(BF16)

    def down(depth, slot, n):
        y = jnp.dot(cu_v[:, :depth], wod_v[:depth, cols(n)], preferred_element_type=F32)
        p_v[slot, :, cols(n)] = y.astype(BF16)

    def pm_copy():
        return remote(p_v.at[0], pm, s_pm.at[0], s_pm.at[1], mate)

    def f_wait(count, group):
        rows = out.at[pl.ds(0, count * ROWS)]
        both = remote(rows, rows, s_f.at[0, group], s_f.at[1, group], mate)
        both.wait_send()
        both.wait_recv()

    in_u, in_od = d_model, 2 * hw

    def final_load(k):
        if k == 0:
            return pltpu.make_async_copy(out.at[pl.ds(0, in_u)], wu_v, s_fin.at[0])
        return pltpu.make_async_copy(out.at[pl.ds(in_u, in_od)], wod_v, s_fin.at[1])

    def send_group(i, k):
        for j in range(2, len(groups)):
            @pl.when((i == j) & (core == twin))
            def _():
                group_send(j, k).start()

    barrier = pltpu.get_barrier_semaphore()
    for d in (inn_d, outn_d, mate, dev(outn, CORES - 1 - core), peer):
        pl.semaphore_signal(barrier, inc=1, device_id=d, device_id_type=MESH)
    x_load(jnp.int32(0))
    tab_copy(jnp.int32(0)).start()
    for g in range(n_slots):
        q_copy(jnp.int32(g)).start()
    pl.semaphore_wait(barrier, 5)

    @pl.when(core == twin)
    def _():
        for j in range(2):
            for k in range(4):
                group_send(j, k).start()

    @pl.loop(0, total + 4)
    def _(i):
        t = i - 1
        tc = jnp.maximum(t, 0)
        compute = i <= total
        small = i < 2
        whole = (i >= 2) & compute
        blk = lax.rem(tc, blocks)
        job = (t - side_at) * 2
        has_jobs = (t >= side_at) & (t < side_at + n_side // 2)

        def on(cond):
            return pl.when(cond)

        @on(i == 0)
        def _():
            load_q()
            clear_tail(slot(1))
            for k in range(2):
                o_copy(w_o.at[0], k, slot(k)).start()
            for c in own_ud(0):
                c.start()

        @on(compute)
        def _():
            x_wait()
            layer_norm(lax.div(tc, items))

            @on(i < total)
            def _():
                x_load(i + 1)

        @on(i == 0)
        def _():
            push(0).start()

        send_group(i, 0)
        for j in range(len(groups)):
            @on((t == j + 1) & (core == 1))
            def _():
                group_bytes(1, s_gx.at[j]).wait_recv()
                for c in group_pass(j):
                    c.start()

        @on(t == items)
        def _():
            for c in second(0):
                c.wait()

        @on(i == 1)
        def _():
            push_kv().wait_send()

        @on(i == 2)
        def _():
            push(0).wait_recv()
            push_kv().wait_recv()

        @on(compute & (i != 1))
        def _():
            tab_copy(blk).wait()

        @on(small)
        def _():
            qkv_half()

        @on(whole)
        def _():
            for g in range(2 * heads):
                qkv(blk, g)

        @on((i >= 1) & (i < total))
        def _():
            tab_copy(lax.rem(i, blocks)).start()

        lagged(phase_b2, t - 1, 1)

        @on((t > side_at) & (t <= side_at + n_side // 2))
        def _():
            side_job(job - 1, 1)

        @on(t == items - 1)
        def _():
            pq_copy(0).wait()
            po_copy(0).wait()
            pl.semaphore_signal(s_rdy, inc=1, device_id=mate, device_id_type=MESH)
            start_second(0)

        send_group(i, 1)

        @on(small)
        def _():
            four_heads(0, ROWS)

        @on(i == 0)
        def _():
            push_kv().start()

        @on(whole)
        def _():
            attention(blk)

        send_group(i, 2)

        @on(compute)
        def _():
            wait_ud(i, 0)

            @on(small)
            def _():
                for n in range(ff // tile):
                    up(0, n)

            @on(whole)
            def _():
                for h in range(2):
                    for n in range(ff // tile):
                        up(h, n)

        @on(has_jobs)
        def _():
            side_copy(job, 0)

        @on(t == items - 1)
        def _():
            weights_here(5, 10, (2,))
            start_second(1)

        @on(t == total - 1)
        def _():
            f_wait(items - late, 0)
            final_load(0).start()

        lagged(phase_e1, t - 5, 0)
        lagged(phase_e2, t - 3, 1)
        lagged(phase_d1, t - 4, 0)
        lagged(phase_d2, t - 2, 1)
        lagged(phase_c1, t - 3, 0)
        lagged(phase_b1, t - 2, 0)
        send_group(i, 3)

        @on(small)
        def _():
            @on(i == 0)
            def _():
                load_o()

            @on(i == 1)
            def _():
                pm_copy().wait_send()

            wait_ud(i, 1)

            @pl.loop(0, d_model // tile, step=2)
            def _(n):
                for k in range(2):
                    down(hw, 0, n + k)

            @on(i == 0)
            def _():
                pm_copy().start()
                for k in range(1, 4):
                    push(k).start()

            @on(i == 1)
            def _():
                pm_copy().wait_recv()

                def add(rows):
                    p_v[0, rows(), :] = (f32(p_v[0, rows(), :]) + f32(pm[rows(), :])).astype(BF16)

                by_rows(ROWS, add)

        @on(i == 2)
        def _():
            push(1).wait_recv()

        @on(whole)
        def _():
            wait_ud(i, 1)
            for n in range(d_model // tile):
                down(2 * hw, s3(t), n)

        lagged(phase_c2, t - 1, 1)

        @on((i >= 1) & compute)
        def _():
            phase_a(t)

        @on(has_jobs)
        def _():
            side_copy(job + 1, 1)
            side_job(job, 0)

        @on(t == items - 1)
        def _():
            weights_here(10, len(groups), (3,))
            start_second(2)

        @on(t == total - 1)
        def _():
            final_load(1).start()

        @on(t == 2)
        def _():
            for k in range(4):
                push(k).wait_send()

            @on(core == 1)
            def _():
                for k in range(4):
                    push2(k).start()

        @on(t == side_at - 1)
        def _():
            weights_here(0, 5, (0, 1))


    @pl.when(core == 1)
    def _():
        for i in range(4):
            push2(i).wait_send()
        group_bytes(1, s_gx.at[0], len(groups)).wait_send()

    @pl.when(core == twin)
    def _():
        group_bytes(0, s_gx.at[0], len(groups)).wait_send()

    f_wait(late, 1)
    for k in range(2):
        final_load(k).wait()


def collect(y, va, vb, out, buf, sem):
    na, nb = va.shape[0], vb.shape[0]
    spans = [pl.ds(na + nb + n * ROWS, ROWS) for n in range(buf.shape[0])]
    ins = [pltpu.make_async_copy(y.at[r], buf.at[n], sem.at[2 + n]) for n, r in enumerate(spans)]
    outs = [pltpu.make_async_copy(buf.at[n], out.at[r], sem.at[2 + n]) for n, r in enumerate(spans)]
    direct = [
        pltpu.make_async_copy(va, out.at[pl.ds(0, na)], sem.at[0]),
        pltpu.make_async_copy(vb, out.at[pl.ds(na, nb)], sem.at[1]),
    ]
    for c in ins + direct:
        c.start()
    for c, d in zip(ins, outs):
        c.wait()
        d.start()
    for c in direct + outs:
        c.wait()


def solution(mesh):
    n_tp = mesh.shape["tp"]
    n_chip = n_tp // CORES

    def shard_body(act_in, ln_gain, ln_bias, w_qkv, w_out, w_up, w_down):
        batch, seq_len, d_model = act_in.shape
        layers, _, heads, group_cols = w_qkv.shape
        head_dim = w_out.shape[1] // heads
        ff = w_up.shape[2]
        assert group_cols == 3 * head_dim and heads == 4 and head_dim == 2 * SLOT
        items = batch * seq_len // (CORES * ROWS)
        blocks = seq_len // ROWS
        late = 4
        cfg = (n_chip, layers, heads, head_dim, d_model, ff, items, blocks, late)
        ow = 4 * LANES
        quart = ROWS // 4
        n_groups = (heads * group_cols + heads * head_dim + d_model // 2 + ff) // ROWS
        w_q = jnp.transpose(w_qkv, (0, 2, 3, 1)).reshape(layers, heads * group_cols, d_model)
        vm = pl.BlockSpec(memory_space=pltpu.VMEM)
        hb = pl.BlockSpec(memory_space=pl.ANY)
        dma = pltpu.SemaphoreType.DMA
        two, three, four, square, pieces4, many = (dma(n) for n in ((2,), (3,), (4,), (2, 2), (4, 2), (n_groups,)))
        plain = pltpu.SemaphoreType.REGULAR
        out_vmem = (d_model * 2 * ff + (2 * ow + 2 * ff) * d_model) * 2
        res = pl.pallas_call(
            functools.partial(body, cfg),
            name="layers",
            out_shape=[
                jax.ShapeDtypeStruct((batch * seq_len, d_model), BF16),
                pltpu.VMEM((d_model, 2 * ff), BF16),
                pltpu.VMEM((2 * ow + 2 * ff, d_model), BF16),
                jax.ShapeDtypeStruct((2, heads * group_cols, d_model), BF16),
                jax.ShapeDtypeStruct((2, heads * head_dim, d_model), BF16),
                jax.ShapeDtypeStruct((2, d_model, ff), BF16),
                jax.ShapeDtypeStruct((2, ff, d_model), BF16),
                jax.ShapeDtypeStruct((2 * heads, d_model, 2 * LANES), BF16),
                jax.ShapeDtypeStruct((2 * ow, d_model), BF16),
            ],
            in_specs=[hb] * 5 + [vm] * 2 + [hb, vm],
            out_specs=[hb, vm, vm] + [hb] * 6,
            scratch_shapes=[
                pltpu.VMEM((ROWS, 2 * LANES), F32),
                pltpu.VMEM((d_model, 2 * LANES), BF16),
                pltpu.VMEM((ROWS, d_model), BF16),
                pltpu.VMEM((ROWS, d_model), BF16),
                pltpu.VMEM((ROWS, d_model), BF16),
                pltpu.VMEM((2 * heads, ROWS, 2 * LANES), BF16),
                pltpu.VMEM((2 * heads, seq_len, 2 * LANES), BF16),
                pltpu.VMEM((ROWS, 2 * ow + 2 * ff), BF16),
                pltpu.VMEM((3, ROWS, d_model), BF16),
                pltpu.VMEM((2 * heads, d_model, 2 * LANES), BF16),
                pltpu.VMEM((3, 2 * quart, d_model), BF16),
                pltpu.VMEM((2 * quart, d_model), BF16),
                pltpu.VMEM((2 * quart, d_model), BF16),
                pltpu.VMEM((2, quart, d_model), BF16),
                pltpu.VMEM((quart, d_model), BF16),
                four, three, two, two, two, square, square, four, pieces4, pieces4, square, pieces4, three, two,
                dma, two, square, square, four, four, four, four,
                two, many, many, three, two, two, three, two,
                dma, two, plain, plain, plain,
            ],
            compiler_params=pltpu.CompilerParams(collective_id=0, has_side_effects=True, vmem_limit_bytes=VMEM_LIMIT - out_vmem),
        )(act_in.reshape(batch * seq_len, d_model), w_q, w_out, w_up, w_down, ln_gain, ln_bias, jnp.asarray(rope_tables(seq_len, head_dim)), jnp.asarray(regroup(head_dim), BF16))
        rest = batch * seq_len // ROWS - (d_model + 2 * ow + 2 * ff) // ROWS
        y = pl.pallas_call(
            collect,
            name="collect",
            out_shape=jax.ShapeDtypeStruct((batch * seq_len, d_model), BF16),
            in_specs=[hb, vm, vm],
            out_specs=hb,
            scratch_shapes=[pltpu.VMEM((rest, ROWS, d_model), BF16), dma((2 + rest,))],
            compiler_params=pltpu.CompilerParams(vmem_limit_bytes=16 << 20),
        )(*res[:3])
        return y.reshape(batch, seq_len, d_model)

    wide = P(None, None, "tp")
    tall = P(None, "tp")
    return jax.shard_map(shard_body, mesh=mesh, in_specs=(P("dp"), P(), P(), wide, tall, wide, tall), out_specs=P("dp"), check_vma=False)
```

```python
import functools

import jax
import jax.numpy as jnp
import numpy as np
from jax import lax
from jax.experimental import pallas as pl
from jax.experimental.pallas import tpu as pltpu
from jax.sharding import PartitionSpec as P

LN_EPS = 1e-5
ROPE_BASE = 10000.0
F32 = jnp.float32
BF16 = jnp.bfloat16
MESH = pl.DeviceIdType.MESH
VMEM_LIMIT = 67043328

CORES = 2
ROWS = 256
LANES = 128
SLOT = 40
LN_ROWS = 128
UNROLLED = 4


def rope_tables(seq_len, head_dim):
    half_dim = head_dim // 2
    inv_freq = (ROPE_BASE ** (-2.0 * np.arange(half_dim, dtype=np.float32) / head_dim)).astype(np.float32)
    angles = np.arange(seq_len, dtype=np.float32)[:, None] * inv_freq[None, :]
    cos_tab = np.ones((seq_len, LANES), np.float32)
    sin_tab = np.zeros((seq_len, LANES), np.float32)
    for k in range(2):
        cos_tab[:, k * half_dim:(k + 1) * half_dim] = np.cos(angles)
        sin_tab[:, k * half_dim:(k + 1) * half_dim] = np.sin(angles)
    return np.concatenate([cos_tab, sin_tab], axis=1)


def regroup(head_dim):
    half_dim = head_dim // 2
    sel = np.zeros((3 * head_dim, 2 * LANES), np.float32)
    for part in range(3):
        for half in range(2):
            for i in range(half_dim):
                sel[(part * 2 + half) * half_dim + i, half * LANES + part * half_dim + i] = 1.0
    return sel


def body(cfg, act, w_q, w_o, w_u, w_d, gain, bias, tab, sel_v,
         out, wu_v, wod_v, st_q, st_o, st_u, st_d, pq, po,
         tab_v, pst, pm, x_v, n_v, q_v, kv_v, cu_v, p_v, wq_v,
         ar, br, ysh, br2, ysh2,
         s_as, s_ar, s_ar2, s_bs, s_br, s_br2, s_cs, s_cr, s_cr2, s_co, s_ds, s_do, s_y1, s_yl, s_x, s_xr, s_f, s_wl, s_ws, s_wr, s_m2s, s_m2r,
         s_gs, s_gx, s_gp, s_stg, s_pm, s_pq, s_rl, s_fin, s_tab, s_kv, s_ca, s_cb, s_rdy):
    n_chip, layers, heads, head_dim, d_model, ff, items, blocks, late = cfg
    side_at = 9
    group_cols = 3 * head_dim
    seq_blocks = blocks
    group_cols = 3 * head_dim
    half_dim = head_dim // 2
    total = layers * items
    tp = lax.axis_index("tp")
    dp = lax.axis_index("dp")
    chip = lax.div(tp, CORES)
    core = lax.rem(tp, CORES)
    twin = lax.rem(dp, 2)
    odd = lax.rem(chip, 2)
    pair = lax.div(chip, 2)
    inn = chip + 1 - 2 * odd
    outn = lax.rem(chip + n_chip - 1 + 2 * odd, n_chip)

    def dev(c, k):
        return {"tp": c * CORES + k}

    inn_d, outn_d, mate = dev(inn, core), dev(outn, core), dev(chip, CORES - 1 - core)
    peer = {"dp": dp + 1 - 2 * twin, "tp": tp}
    own_base = core * (items * ROWS)
    mate_base = (CORES - 1 - core) * (items * ROWS)
    half = ROWS // 2
    quart = ROWS // 4
    ow = 4 * LANES
    hw = ow + ff

    def remote(src, dst, ssem, rsem, dev):
        return pltpu.make_async_remote_copy(src_ref=src, dst_ref=dst, send_sem=ssem, recv_sem=rsem, device_id=dev, device_id_type=MESH)

    def at(base, off, size):
        return pl.ds(pl.multiple_of(base + off, min(size, quart)), size)

    def rows1(t, off, size):
        return at(own_base + lax.rem(t, items) * ROWS, off, size)

    def rows2(t, p, off, size):
        u = t - items
        q = lax.div(u, blocks)
        cc = lax.rem(q, CORES)
        seq = p + cc - 2 * p * cc + 2 * lax.div(q, CORES)
        return at(cc * (items * ROWS) + (seq * blocks + lax.rem(u, blocks)) * ROWS, off, size)

    def owner(t):
        return lax.rem(lax.div(t, blocks) + core, 2) == pair

    def ud_dst(h):
        return [wu_v.at[:, pl.ds(h * ff, ff)], wod_v.at[pl.ds(h * hw + ow, ff)]]

    def own_ud(l):
        return [pltpu.make_async_copy(s.at[l], d, s_wl.at[0, i]) for i, (s, d) in enumerate(zip((w_u, w_d), ud_dst(0)))]

    def staged_ud(h):
        return [pltpu.make_async_copy(s.at[h], d, s_wl.at[h, i]) for i, (s, d) in enumerate(zip((st_u, st_d), ud_dst(h)))]

    def push(i):
        src = (wq_v.at[pl.ds(0, heads)], wod_v.at[pl.ds(0, ow)], w_u.at[0], w_d.at[0])[i]
        dst = (wq_v.at[pl.ds(heads, heads)], wod_v.at[pl.ds(hw, ow)], *ud_dst(1))[i]
        return remote(src, dst, s_ws.at[i], s_wr.at[i], mate)

    def push_kv():
        rows = pl.ds(0, ROWS)
        return remote(kv_v.at[pl.ds(0, heads), rows], kv_v.at[pl.ds(heads, heads), rows], s_kv.at[0], s_kv.at[1], mate)

    args2 = (w_q.at[1], w_o.at[1], w_u.at[1], w_d.at[1])
    staged = (st_q, st_o, st_u, st_d)

    def push2(i):
        return remote(args2[i], staged[i].at[1], s_m2s.at[i], s_m2r.at[i], mate)

    pieces = []
    for k, (n_rows, step) in enumerate(((heads * group_cols, quart), (heads * head_dim, quart), (d_model, 2 * quart), (ff, quart))):
        pieces += [(k, r, step) for r in range(0, n_rows, step)]
    groups = [pieces[j:j + 4] for j in range(0, len(pieces), 4)]

    def group_send(j, k):
        arr, r, n = groups[j][k]
        rows = pl.ds(r, n)
        return remote(args2[arr].at[rows], staged[arr].at[twin, rows], s_gs.at[0], s_gx.at[j], dev(outn, 1))

    def group_pass(j):
        copies = []
        for arr in range(4):
            mine = [p for p in groups[j] if p[0] == arr]
            if mine:
                rows = pl.ds(mine[0][1], sum(p[2] for p in mine))
                copies.append(remote(staged[arr].at[twin, rows], staged[arr].at[twin, rows], s_gs.at[1], s_gp.at[j], peer))
        return copies

    def group_bytes(j, sem, n=1):
        rows = out.at[pl.ds(0, n * ROWS)]
        return remote(rows, rows, s_gs.at[j], sem, peer)

    def regroup_q(src, dst, unroll=False):
        def one(c):
            part = pl.ds(c, 512) if unroll else pl.ds(pl.multiple_of(c, 512), 512)
            y = lax.dot_general(src[:, part], sel_v[...], (((0,), (0,)), ((), ())), preferred_element_type=F32)
            dst[part, :] = y.astype(BF16)

        if unroll:
            for c in range(0, d_model, 512):
                one(c)
        else:
            pl.loop(0, d_model, step=512)(one)

    def regroup_o(src, dst, unroll=False):
        def one(c):
            part = pl.ds(c, 512) if unroll else pl.ds(pl.multiple_of(c, 512), 512)
            y = lax.dot_general(sel_v[...], src[:, part], (((0,), (0,)), ((), ())), preferred_element_type=F32)
            dst[:, part] = y.astype(BF16)

        if unroll:
            for c in range(0, d_model, 512):
                one(c)
        else:
            pl.loop(0, d_model, step=512)(one)

    def slot(k):
        return p_v.at[k, pl.ds(0, group_cols)]

    n_slots = 3

    def q_copy(g):
        rows = pl.ds(pl.multiple_of(g * group_cols, group_cols), group_cols)
        k = lax.rem(g, n_slots)
        return pltpu.make_async_copy(w_q.at[0, rows], slot(k), s_stg.at[k])

    def load_q():
        @pl.loop(0, heads)
        def _(g):
            q_copy(g).wait()
            regroup_q(slot(lax.rem(g, n_slots)), wq_v.at[g], True)

            @pl.when(g + n_slots < heads)
            def _():
                q_copy(g + n_slots).start()

    def o_copy(src, k, dst):
        rows = (pl.ds(0, group_cols), pl.ds(group_cols, head_dim))[k]
        return pltpu.make_async_copy(src.at[rows], dst.at[pl.ds(0, (group_cols, head_dim)[k])], s_stg.at[k])

    def clear_tail(ref):
        ref[pl.ds(head_dim, group_cols - head_dim), :] = jnp.zeros((group_cols - head_dim, d_model), BF16)

    def load_o():
        for k in range(2):
            o_copy(w_o.at[0], k, slot(k)).wait()

        @pl.loop(0, 2)
        def _(k):
            regroup_o(slot(k), wod_v.at[pl.ds(pl.multiple_of(k * 2 * LANES, 2 * LANES), 2 * LANES)], True)

    n_side = 2 * heads + 4
    side_refs = (n_v.at[pl.ds(0, group_cols)], cu_v.at[pl.ds(0, group_cols), pl.ds(0, d_model)])

    def side_copy(a, k):
        for h in range(2):
            for arg in range(2 - h):
                from_arg = (core == 0) if arg else ((core == 1) if h == 0 else (core >= 0))

                @pl.when((a >= h * heads) & (a < (h + 1) * heads) & from_arg)
                def _():
                    rows = pl.ds(pl.multiple_of((a - h * heads) * group_cols, group_cols), group_cols)
                    src = w_q.at[1, rows] if arg else st_q.at[h, rows]
                    pltpu.make_async_copy(src, side_refs[k], s_stg.at[k]).start()

                @pl.when((a == 2 * heads + 2 * h + k) & from_arg)
                def _():
                    if k:
                        clear_tail(side_refs[k])
                    o_copy(w_o.at[1] if arg else st_o.at[h], k, side_refs[k]).start()

    def pq_copy(g):
        return pltpu.make_async_copy(pst, pq.at[g], s_pq.at[0])

    def po_copy(b):
        return pltpu.make_async_copy(pm, po.at[pl.ds(pl.multiple_of(b * 2 * LANES, 2 * LANES), 2 * LANES)], s_pq.at[1])

    def side_job(a, k):
        @pl.when(a < 2 * heads)
        def _():
            pltpu.make_async_copy(w_q.at[1, pl.ds(0, group_cols)], side_refs[k], s_stg.at[k]).wait()

            @pl.when(a > 0)
            def _():
                pq_copy(a - 1).wait()

            regroup_q(side_refs[k], pst)
            pq_copy(a).start()

        @pl.when(a >= 2 * heads)
        def _():
            o_copy(w_o.at[1], k, side_refs[k]).wait()

            @pl.when(a > 2 * heads)
            def _():
                po_copy(a - 2 * heads - 1).wait()

            regroup_o(side_refs[k], pm)
            po_copy(a - 2 * heads).start()

    def start_second(k):
        if k == 0:
            second(0)[0].start()
            return

        @pl.when(core == 0)
        def _():
            own_ud(1)[k - 1].start()

        @pl.when(core == 1)
        def _():
            staged_ud(0)[k - 1].start()

        for c in second(k)[1:]:
            c.start()

    def second(k):
        if k == 0:
            return [pltpu.make_async_copy(pq, wq_v, s_rl.at[0])]
        outs = [pltpu.make_async_copy(po.at[pl.ds(h * ow, ow)], wod_v.at[pl.ds(h * hw, ow)], s_rl.at[1 + h]) for h in range(2)]
        return [staged_ud(h)[k - 1] for h in range(2)] + (outs if k == 2 else [])

    def wait_ud(i, k):
        @pl.when(i == 0)
        def _():
            own_ud(0)[k].wait()

        @pl.when(i == 2)
        def _():
            push(2 + k).wait_recv()

        @pl.when(i == items + 1)
        def _():
            for c in second(1 + k):
                c.wait()

    def weights_here(first, last, mate_pieces):
        @pl.when(core == 0)
        def _():
            for k in mate_pieces:
                push2(k).wait_recv()

        @pl.when(core == 1)
        def _():
            for j in range(first, last):
                group_bytes(0, s_gp.at[j]).wait_recv()

    def x_load(i):
        t = i - 1

        @pl.when(i == 0)
        def _():
            pltpu.make_async_copy(act.at[pl.ds(pl.multiple_of(mate_base, ROWS), ROWS)], x_v, s_x).start()

        @pl.when((i >= 1) & (t < items))
        def _():
            pltpu.make_async_copy(act.at[rows1(t, 0, ROWS)], x_v, s_x).start()

        @pl.when(t >= items)
        def _():
            q = lax.div(t - items, blocks)

            @pl.when((lax.rem(t, blocks) == 0) & (lax.rem(q, CORES) != core))
            def _():
                seq = out.at[pl.ds(0, blocks * ROWS)]
                remote(seq, seq, s_y1.at[0], s_y1.at[1 + lax.div(q, CORES)], mate).wait_recv()

            pltpu.make_async_copy(out.at[rows2(t, pair, 0, ROWS)], x_v, s_x).start()

    def x_wait():
        pltpu.make_async_copy(act.at[pl.ds(0, ROWS)], x_v, s_x).wait()

    def sl(t):
        return lax.rem(t, 2)

    def s3(t):
        return lax.rem(t, 3)

    def nth(t):
        return lax.div(t, 2 * blocks) * blocks + lax.rem(t, blocks)

    def prow(t, off, size):
        return (s3(t), at(0, off, size))

    def a1(t):
        off = jnp.where(owner(t), 1 - odd, odd) * half
        return remote(p_v.at[prow(t, off, half)], ar.at[s3(t)], s_as.at[s3(t)], s_ar.at[s3(t)], inn_d)

    def b1(t):
        return remote(ar.at[s3(t)], br, s_bs.at[0], s_br.at[0], outn_d)

    def c1(t):
        rows = rows1(t, odd * half, half)
        return [
            remote(ysh, out.at[rows], s_cs.at[0, 0], s_cr.at[lax.rem(t, 4)], inn_d),
            remote(ysh, out.at[rows], s_cs.at[0, 1], s_y1.at[1 + lax.div(t, 2 * blocks)], mate),
        ]

    def l1(t):
        return pltpu.make_async_copy(ysh, out.at[rows1(t, odd * half, half)], s_yl.at[0])

    def d1(t):
        rows = rows1(t, (1 - odd) * half, half)
        return remote(out.at[rows], out.at[rows], s_ds.at[0, sl(t)], s_y1.at[1 + lax.div(t, 2 * blocks)], mate)

    def r1(t):
        return pltpu.make_async_copy(act.at[rows1(t, odd * half, half)], ysh, s_xr.at[0])

    def a2(t):
        return remote(p_v.at[prow(t, (1 - core) * half, half)], pm.at[at(0, sl(t) * half, half)], s_as.at[3], s_ar2.at[sl(t)], mate)

    piece = quart // 2

    def b2(t, p):
        m = sl(t) * half + (1 - odd) * quart
        dst = br2.at[sl(t), pl.ds(p * piece, piece)]
        return remote(pm.at[piece_rows(m, p)], dst, s_bs.at[1], s_br2.at[sl(t), p], inn_d)

    def piece_rows(base, p):
        return pl.ds(pl.multiple_of(base + p * piece, piece), piece)

    def c2(t, p):
        rows = rows2(t, pair, core * half + odd * quart + p * piece, piece)
        src = ysh2.at[pl.ds(p * piece, piece)]
        k = lax.rem(t, 4)
        return [
            remote(src, out.at[rows], s_cs.at[1, 0], s_cr2.at[k, p], inn_d),
            remote(src, out.at[rows], s_cs.at[1, 1], s_co.at[k, p], outn_d),
        ]

    def l2(t):
        return pltpu.make_async_copy(ysh2, out.at[rows2(t, pair, core * half + odd * quart, quart)], s_yl.at[1])

    def d2(t, p):
        rows = rows2(t, pair, core * half + (1 - odd) * quart + p * piece, piece)
        return remote(out.at[rows], out.at[rows], s_ds.at[1, sl(t)], s_do.at[lax.rem(t, 4), p], outn_d)

    def sent2(sem):
        return remote(ysh2, ysh2, sem, s_cr2.at[0, 0], inn_d).wait_send()

    def r2(t):
        return pltpu.make_async_copy(out.at[rows2(t, pair, core * half + odd * quart, quart)], ysh2, s_xr.at[1])

    def f2(t, group):
        copies = []
        for p in (pair, 1 - pair):
            rows = rows2(t, p, core * half, half)
            copies.append(remote(out.at[rows], out.at[rows], s_f.at[0, group], s_f.at[1, group], mate))
        return copies

    def f32(x):
        return x.astype(F32)

    def by_rows(n, f):
        @pl.loop(0, n // 16)
        def _(i):
            f(lambda base=0: pl.ds(pl.multiple_of(base + i * 16, 16), 16))

    def slot_free(t):
        @pl.when(t + 3 < items)
        def _():
            pl.semaphore_signal(s_ca, inc=1, device_id=inn_d, device_id_type=MESH)

    def phase_a(t):
        @pl.when(t < items)
        def _():
            @pl.when(t >= 3)
            def _():
                pl.semaphore_wait(s_ca, 1)

            a1(t).start()

            @pl.when((t == 0) & owner(t))
            def _():
                r1(t).start()

        @pl.when(t >= items)
        def _():
            @pl.when(t == items)
            def _():
                pl.semaphore_wait(s_rdy, 1)

            a2(t).start()

            @pl.when(t == items)
            def _():
                r2(t).start()

    def phase_b1(t):
        @pl.when(jnp.logical_not(owner(t)))
        def _():
            n = nth(t)

            @pl.when(n > 0)
            def _():
                pl.semaphore_wait(s_cb, 1)

            a1(t).wait_recv()
            k = s3(t)

            def add(rows):
                ar[k, rows(), :] = (f32(p_v[k, rows((1 - odd) * half), :]) + f32(ar[k, rows(), :])).astype(BF16)

            by_rows(half, add)
            b1(t).start()

    def phase_c1(t):
        a1(t).wait_send()

        @pl.when(jnp.logical_not(owner(t)))
        def _():
            b1(t).wait_send()
            slot_free(t)

        @pl.when(owner(t))
        def _():
            a1(t).wait_recv()
            b1(t).wait_recv()
            r1(t).wait()
            k = s3(t)

            def add(rows):
                summed = f32(p_v[k, rows(odd * half), :]) + f32(ar[k, rows(), :]) + f32(br[rows(), :])
                ysh[rows(), :] = (f32(ysh[rows(), :]) + f32(summed.astype(BF16))).astype(BF16)

            by_rows(half, add)
            slot_free(t)

            @pl.when(nth(t) + 1 < items // 2)
            def _():
                pl.semaphore_signal(s_cb, inc=1, device_id=outn_d, device_id_type=MESH)

            for c in c1(t):
                c.start()
            l1(t).start()

    def phase_d1(t):
        @pl.when(owner(t))
        def _():
            c1(t)[0].wait_recv()
            l1(t).wait()
            for c in c1(t):
                c.wait_send()
            d1(t).start()

        @pl.when((t + 1 < items) & owner(t + 1))
        def _():
            r1(t + 1).start()

    def phase_e1(t):
        @pl.when(owner(t))
        def _():
            d1(t).wait_send()

    def phase_b2(t):
        a2(t).wait_recv()
        k, m = s3(t), sl(t) * half
        for p in range(2):
            q = (1 - odd) * quart + p * piece

            def add(rows):
                pm[rows(m + q), :] = (f32(p_v[k, rows(core * half + q), :]) + f32(pm[rows(m + q), :])).astype(BF16)

            by_rows(piece, add)
            b2(t, p).start()

    def phase_c2(t):
        a2(t).wait_send()
        r2(t).wait()
        k, k2, m = s3(t), sl(t), sl(t) * half
        for p in range(2):
            q = odd * quart + p * piece
            o = p * piece

            def add(rows):
                summed = f32(p_v[k, rows(core * half + q), :]) + f32(pm[rows(m + q), :]) + f32(br2[k2, rows(o), :])
                ysh2[rows(o), :] = (f32(ysh2[rows(o), :]) + f32(summed.astype(BF16))).astype(BF16)

            b2(t, p).wait_recv()
            by_rows(piece, add)
            for c in c2(t, p):
                c.start()
        l2(t).start()
        sent2(s_bs.at[1])

    def phase_d2(t):
        for p in range(2):
            c2(t, p)[0].wait_recv()
            d2(t, p).start()
        l2(t).wait()
        for k in range(2):
            sent2(s_cs.at[1, k])

        @pl.when(t + 1 < total)
        def _():
            r2(t + 1).start()

    def phase_e2(t):
        sent2(s_ds.at[1, sl(t)])
        for p in range(2):
            c2(t, p)[1].wait_recv()
            d2(t, p).wait_recv()

        @pl.when(t < total - late)
        def _():
            for c in f2(t, 0):
                c.start()

        @pl.when(t >= total - late)
        def _():
            for c in f2(t, 1):
                c.start()

    def lagged(phase, t, layer):
        lo, hi = layer * items, (layer + 1) * items

        @pl.when((t >= lo) & (t < hi))
        def _():
            phase(t)

    lane = lax.broadcasted_iota(jnp.int32, (ROWS, LANES), 1)

    def layer_norm(l):
        step = LN_ROWS

        @pl.loop(0, ROWS // step)
        def _(i):
            r = pl.ds(pl.multiple_of(i * step, step), step)
            xf = x_v[r, :].astype(F32)
            mean = jnp.mean(xf, axis=-1, keepdims=True)
            centered = xf - mean
            var = jnp.mean(centered * centered, axis=-1, keepdims=True)
            n_v[r, :] = (centered * lax.rsqrt(var + LN_EPS) * gain[pl.ds(l, 1), :] + bias[pl.ds(l, 1), :]).astype(BF16)

    def tab_copy(blk):
        return pltpu.make_async_copy(tab.at[pl.ds(pl.multiple_of(blk * ROWS, ROWS), ROWS)], tab_v, s_tab)

    def qkv(blk, g):
        rows = pl.ds(pl.multiple_of(blk * ROWS, ROWS), ROWS)
        y = jnp.dot(n_v[...], wq_v[g], preferred_element_type=F32)
        t0, t1 = y[:, :LANES], y[:, LANES:]
        cs, sn = tab_v[:, :LANES], tab_v[:, LANES:]
        for k, v in enumerate((t0 * cs - t1 * sn, t1 * cs + t0 * sn)):
            cols = pl.ds(k * LANES, LANES)
            q_v[g, :, cols] = jnp.where(lane < half_dim, v, 0.0).astype(BF16)
            kv_v[g, rows, cols] = pltpu.roll(v, LANES - half_dim, 1).astype(BF16)

    def qkv_half():
        for g in range(heads):
            qkv(jnp.int32(0), g)

    def attend(g, n):
        scores = lax.dot_general(q_v[g], kv_v[g, :n, :], (((1,), (1,)), ((), ())), preferred_element_type=F32)
        ri = lax.broadcasted_iota(jnp.int32, (ROWS, ROWS), 0)
        ci = lax.broadcasted_iota(jnp.int32, (ROWS, ROWS), 1)
        diag = jnp.where(ri >= ci, scores[:, n - ROWS:], -1e30)
        scores = jnp.concatenate([scores[:, :n - ROWS], diag], axis=1) if n > ROWS else diag
        e = jnp.exp2((scores - jnp.max(scores, axis=1, keepdims=True)) * np.float32(head_dim ** -0.5 * np.log2(np.e)))
        probs = (e * (1.0 / jnp.sum(e, axis=1, keepdims=True))).astype(BF16)
        return jnp.dot(probs, kv_v[g, :n, :], preferred_element_type=F32)

    def four_heads(h, n):
        base = h * hw
        ctx = [attend(h * heads + j, n) for j in range(heads)]
        for k in range(2):
            first, second, third, fourth = (c[:, k * LANES:(k + 1) * LANES] for c in ctx)
            v = jnp.where(lane < half_dim, pltpu.roll(first, LANES - half_dim, 1), second)
            w = jnp.where(lane < 3 * half_dim, pltpu.roll(third, half_dim, 1), 0.0)
            cu_v[:, pl.ds(pl.multiple_of(base + k * LANES, LANES), LANES)] = jnp.where(lane < 2 * half_dim, v, w).astype(BF16)
            v = jnp.where(lane < half_dim, pltpu.roll(fourth, LANES - half_dim, 1), 0.0)
            cu_v[:, pl.ds(pl.multiple_of(base + (2 + k) * LANES, LANES), LANES)] = v.astype(BF16)

    def attention(blk):
        for i in range(blocks):
            @pl.when(blk == i)
            def _():
                if i < UNROLLED:
                    for h in range(2):
                        four_heads(h, (i + 1) * ROWS)
                else:
                    pl.loop(0, 2)(lambda h: four_heads(h, (i + 1) * ROWS))

    tile = 2 * LANES

    def cols(n):
        return pl.ds(pl.multiple_of(n * tile, tile), tile)

    def up(h, n):
        y = jnp.dot(n_v[...], wu_v[:, cols(h * (ff // tile) + n)], preferred_element_type=F32)
        u = 0.5 * y * (1.0 + lax.erf(y * np.float32(0.5 ** 0.5)))
        cu_v[:, cols((h * hw + ow) // tile + n)] = u.astype(BF16)

    def down(depth, slot, n):
        y = jnp.dot(cu_v[:, :depth], wod_v[:depth, cols(n)], preferred_element_type=F32)
        p_v[slot, :, cols(n)] = y.astype(BF16)

    def pm_copy():
        return remote(p_v.at[0], pm, s_pm.at[0], s_pm.at[1], mate)

    def f_wait(count, group):
        rows = out.at[pl.ds(0, count * ROWS)]
        both = remote(rows, rows, s_f.at[0, group], s_f.at[1, group], mate)
        both.wait_send()
        both.wait_recv()

    in_u, in_od = d_model, 2 * hw

    def final_load(k):
        if k == 0:
            return pltpu.make_async_copy(out.at[pl.ds(0, in_u)], wu_v, s_fin.at[0])
        return pltpu.make_async_copy(out.at[pl.ds(in_u, in_od)], wod_v, s_fin.at[1])

    def send_group(i, k):
        for j in range(2, len(groups)):
            @pl.when((i == j) & (core == twin))
            def _():
                group_send(j, k).start()

    barrier = pltpu.get_barrier_semaphore()
    for d in (inn_d, outn_d, mate, dev(outn, CORES - 1 - core), peer):
        pl.semaphore_signal(barrier, inc=1, device_id=d, device_id_type=MESH)
    x_load(jnp.int32(0))
    tab_copy(jnp.int32(0)).start()
    for g in range(n_slots):
        q_copy(jnp.int32(g)).start()
    pl.semaphore_wait(barrier, 5)

    @pl.when(core == twin)
    def _():
        for j in range(2):
            for k in range(4):
                group_send(j, k).start()

    @pl.loop(0, total + 4)
    def _(i):
        t = i - 1
        tc = jnp.maximum(t, 0)
        compute = i <= total
        small = i < 2
        whole = (i >= 2) & compute
        blk = lax.rem(tc, blocks)
        job = (t - side_at) * 2
        has_jobs = (t >= side_at) & (t < side_at + n_side // 2)

        def on(cond):
            return pl.when(cond)

        @on(i == 0)
        def _():
            load_q()
            clear_tail(slot(1))
            for k in range(2):
                o_copy(w_o.at[0], k, slot(k)).start()
            for c in own_ud(0):
                c.start()

        @on(compute)
        def _():
            x_wait()
            layer_norm(lax.div(tc, items))

            @on(i < total)
            def _():
                x_load(i + 1)

        @on(i == 0)
        def _():
            push(0).start()

        send_group(i, 0)
        for j in range(len(groups)):
            @on((t == j + 1) & (core == 1))
            def _():
                group_bytes(1, s_gx.at[j]).wait_recv()
                for c in group_pass(j):
                    c.start()

        @on(t == items)
        def _():
            for c in second(0):
                c.wait()

        @on(i == 1)
        def _():
            push_kv().wait_send()

        @on(i == 2)
        def _():
            push(0).wait_recv()
            push_kv().wait_recv()

        @on(compute & (i != 1))
        def _():
            tab_copy(blk).wait()

        @on(small)
        def _():
            qkv_half()

        @on(whole)
        def _():
            for g in range(2 * heads):
                qkv(blk, g)

        @on((i >= 1) & (i < total))
        def _():
            tab_copy(lax.rem(i, blocks)).start()

        lagged(phase_b2, t - 1, 1)

        @on((t > side_at) & (t <= side_at + n_side // 2))
        def _():
            side_job(job - 1, 1)

        @on(t == items - 1)
        def _():
            pq_copy(0).wait()
            po_copy(0).wait()
            pl.semaphore_signal(s_rdy, inc=1, device_id=mate, device_id_type=MESH)
            start_second(0)

        send_group(i, 1)

        @on(small)
        def _():
            four_heads(0, ROWS)

        @on(i == 0)
        def _():
            push_kv().start()

        @on(whole)
        def _():
            attention(blk)

        send_group(i, 2)

        @on(compute)
        def _():
            wait_ud(i, 0)

            @on(small)
            def _():
                for n in range(ff // tile):
                    up(0, n)

            @on(whole)
            def _():
                for h in range(2):
                    for n in range(ff // tile):
                        up(h, n)

        @on(has_jobs)
        def _():
            side_copy(job, 0)

        @on(t == items - 1)
        def _():
            weights_here(5, 10, (2,))
            start_second(1)

        @on(t == total - 1)
        def _():
            f_wait(items - late, 0)
            final_load(0).start()

        lagged(phase_e1, t - 5, 0)
        lagged(phase_e2, t - 3, 1)
        lagged(phase_d1, t - 4, 0)
        lagged(phase_d2, t - 2, 1)
        lagged(phase_c1, t - 3, 0)
        lagged(phase_b1, t - 2, 0)
        send_group(i, 3)

        @on(small)
        def _():
            @on(i == 0)
            def _():
                load_o()

            @on(i == 1)
            def _():
                pm_copy().wait_send()

            wait_ud(i, 1)

            @pl.loop(0, d_model // tile, step=2)
            def _(n):
                for k in range(2):
                    down(hw, 0, n + k)

            @on(i == 0)
            def _():
                pm_copy().start()
                for k in range(1, 4):
                    push(k).start()

            @on(i == 1)
            def _():
                pm_copy().wait_recv()

                def add(rows):
                    p_v[0, rows(), :] = (f32(p_v[0, rows(), :]) + f32(pm[rows(), :])).astype(BF16)

                by_rows(ROWS, add)

        @on(i == 2)
        def _():
            push(1).wait_recv()

        @on(whole)
        def _():
            wait_ud(i, 1)
            for n in range(d_model // tile):
                down(2 * hw, s3(t), n)

        lagged(phase_c2, t - 1, 1)

        @on((i >= 1) & compute)
        def _():
            phase_a(t)

        @on(has_jobs)
        def _():
            side_copy(job + 1, 1)
            side_job(job, 0)

        @on(t == items - 1)
        def _():
            weights_here(10, len(groups), (3,))
            start_second(2)

        @on(t == total - 1)
        def _():
            final_load(1).start()

        @on(t == 2)
        def _():
            for k in range(4):
                push(k).wait_send()

            @on(core == 1)
            def _():
                for k in range(4):
                    push2(k).start()

        @on(t == side_at - 1)
        def _():
            weights_here(0, 5, (0, 1))


    @pl.when(core == 1)
    def _():
        for i in range(4):
            push2(i).wait_send()
        group_bytes(1, s_gx.at[0], len(groups)).wait_send()

    @pl.when(core == twin)
    def _():
        group_bytes(0, s_gx.at[0], len(groups)).wait_send()

    f_wait(late, 1)
    for k in range(2):
        final_load(k).wait()


def collect(y, va, vb, out, buf, sem):
    na, nb = va.shape[0], vb.shape[0]
    spans = [pl.ds(na + nb + n * ROWS, ROWS) for n in range(buf.shape[0])]
    ins = [pltpu.make_async_copy(y.at[r], buf.at[n], sem.at[2 + n]) for n, r in enumerate(spans)]
    outs = [pltpu.make_async_copy(buf.at[n], out.at[r], sem.at[2 + n]) for n, r in enumerate(spans)]
    direct = [
        pltpu.make_async_copy(va, out.at[pl.ds(0, na)], sem.at[0]),
        pltpu.make_async_copy(vb, out.at[pl.ds(na, nb)], sem.at[1]),
    ]
    for c in ins + direct:
        c.start()
    for c, d in zip(ins, outs):
        c.wait()
        d.start()
    for c in direct + outs:
        c.wait()


def solution(mesh):
    n_tp = mesh.shape["tp"]
    n_chip = n_tp // CORES

    def shard_body(act_in, ln_gain, ln_bias, w_qkv, w_out, w_up, w_down):
        batch, seq_len, d_model = act_in.shape
        layers, _, heads, group_cols = w_qkv.shape
        head_dim = w_out.shape[1] // heads
        ff = w_up.shape[2]
        assert group_cols == 3 * head_dim and heads == 4 and head_dim == 2 * SLOT
        items = batch * seq_len // (CORES * ROWS)
        blocks = seq_len // ROWS
        late = 4
        cfg = (n_chip, layers, heads, head_dim, d_model, ff, items, blocks, late)
        ow = 4 * LANES
        quart = ROWS // 4
        n_groups = (heads * group_cols + heads * head_dim + d_model // 2 + ff) // ROWS
        w_q = jnp.transpose(w_qkv, (0, 2, 3, 1)).reshape(layers, heads * group_cols, d_model)
        vm = pl.BlockSpec(memory_space=pltpu.VMEM)
        hb = pl.BlockSpec(memory_space=pl.ANY)
        dma = pltpu.SemaphoreType.DMA
        two, three, four, square, pieces4, many = (dma(n) for n in ((2,), (3,), (4,), (2, 2), (4, 2), (n_groups,)))
        plain = pltpu.SemaphoreType.REGULAR
        out_vmem = (d_model * 2 * ff + (2 * ow + 2 * ff) * d_model) * 2
        res = pl.pallas_call(
            functools.partial(body, cfg),
            name="layers",
            out_shape=[
                jax.ShapeDtypeStruct((batch * seq_len, d_model), BF16),
                pltpu.VMEM((d_model, 2 * ff), BF16),
                pltpu.VMEM((2 * ow + 2 * ff, d_model), BF16),
                jax.ShapeDtypeStruct((2, heads * group_cols, d_model), BF16),
                jax.ShapeDtypeStruct((2, heads * head_dim, d_model), BF16),
                jax.ShapeDtypeStruct((2, d_model, ff), BF16),
                jax.ShapeDtypeStruct((2, ff, d_model), BF16),
                jax.ShapeDtypeStruct((2 * heads, d_model, 2 * LANES), BF16),
                jax.ShapeDtypeStruct((2 * ow, d_model), BF16),
            ],
            in_specs=[hb] * 5 + [vm] * 2 + [hb, vm],
            out_specs=[hb, vm, vm] + [hb] * 6,
            scratch_shapes=[
                pltpu.VMEM((ROWS, 2 * LANES), F32),
                pltpu.VMEM((d_model, 2 * LANES), BF16),
                pltpu.VMEM((ROWS, d_model), BF16),
                pltpu.VMEM((ROWS, d_model), BF16),
                pltpu.VMEM((ROWS, d_model), BF16),
                pltpu.VMEM((2 * heads, ROWS, 2 * LANES), BF16),
                pltpu.VMEM((2 * heads, seq_len, 2 * LANES), BF16),
                pltpu.VMEM((ROWS, 2 * ow + 2 * ff), BF16),
                pltpu.VMEM((3, ROWS, d_model), BF16),
                pltpu.VMEM((2 * heads, d_model, 2 * LANES), BF16),
                pltpu.VMEM((3, 2 * quart, d_model), BF16),
                pltpu.VMEM((2 * quart, d_model), BF16),
                pltpu.VMEM((2 * quart, d_model), BF16),
                pltpu.VMEM((2, quart, d_model), BF16),
                pltpu.VMEM((quart, d_model), BF16),
                four, three, two, two, two, square, square, four, pieces4, pieces4, square, pieces4, three, two,
                dma, two, square, square, four, four, four, four,
                two, many, many, three, two, two, three, two,
                dma, two, plain, plain, plain,
            ],
            compiler_params=pltpu.CompilerParams(collective_id=0, has_side_effects=True, vmem_limit_bytes=VMEM_LIMIT - out_vmem),
        )(act_in.reshape(batch * seq_len, d_model), w_q, w_out, w_up, w_down, ln_gain, ln_bias, jnp.asarray(rope_tables(seq_len, head_dim)), jnp.asarray(regroup(head_dim), BF16))
        rest = batch * seq_len // ROWS - (d_model + 2 * ow + 2 * ff) // ROWS
        y = pl.pallas_call(
            collect,
            name="collect",
            out_shape=jax.ShapeDtypeStruct((batch * seq_len, d_model), BF16),
            in_specs=[hb, vm, vm],
            out_specs=hb,
            scratch_shapes=[pltpu.VMEM((rest, ROWS, d_model), BF16), dma((2 + rest,))],
            compiler_params=pltpu.CompilerParams(vmem_limit_bytes=16 << 20),
        )(*res[:3])
        return y.reshape(batch, seq_len, d_model)

    wide = P(None, None, "tp")
    tall = P(None, "tp")
    return jax.shard_map(shard_body, mesh=mesh, in_specs=(P("dp"), P(), P(), wide, tall, wide, tall), out_specs=P("dp"), check_vma=False)
```
